128 devices in a mesh: chan: 4 (over x), rows: 32 (over z, y, core).
Axes of the slice: x: 4, y: 4, z: 4, core: 2. Of those that a mesh axis runs over, the one named last changes fastest.
Arguments:
- residual: float32 [4, 1024, 16384], P('chan', 'rows'), may hold values from -6 to 6
- psf: float32 [4, 2048, 2048], P('chan', 'rows'), may hold values from -2 to 2
- positions: int32 [32, 2], replicated, may hold values from 0 to 15360, as said below
Outputs:
- residual_out: float32 [4, 1024, 16384], P('chan', 'rows')
- normalized: float32 [1024, 16384], P('rows', 'chan')
The draws below stay inside these ranges and needn't reach their ends.
Inputs may be any that keep to these rules, and one draw needn't show every extreme that they name: positions[k, 0] is a row of the image, 0 to 1023; positions[k, 1] is a column from 1024 to 15360.
All inputs are finite; a program needn't handle non-finite values.
Results may differ from the reference program's by a relative error of at most 0.0001.
Values sent between devices are 32-bit elements; how exact they have to be, the bound alone decides.
No kernel may reach another device: no remote copies, remote signals or barrier semaphores. Data moves between devices by JAX's collectives and lax.ppermute only.
A program may use at most 128 MiB of HBM per device.

```python
import jax
import jax.numpy as jnp
from jax import lax

CHANNELS = 4
NCOL = 16384
PATCH = 2048
STEPS = 32
NX = 1024


def draw_positions(key, part):
    half = PATCH // 2
    row_key = jax.random.fold_in(key, 11)
    col_key = jax.random.fold_in(key, 12)
    pick_key = jax.random.fold_in(key, 13)
    rows = jax.random.randint(row_key, (STEPS,), 0, NX)
    cols = jax.random.randint(col_key, (STEPS,), half, NCOL - half + 1)
    picks = jax.random.randint(pick_key, (2,), 0, STEPS)
    low_step = picks[0]
    high_step = (low_step + 1) % STEPS
    rows = rows.at[low_step].set(0)
    rows = rows.at[high_step].set(NX - 1)
    cols = cols.at[picks[1]].set(NCOL - half)
    return jnp.stack([rows, cols], axis=1).astype(jnp.int32)


def block_scale(key, shape, shards, least, largest):
    factor_of, own = 1.0, jax.random.fold_in(key, 6)
    for axis_at, parts in shards:
        draws = jnp.exp(jax.random.uniform(jax.random.fold_in(own, axis_at), (parts,), jnp.float32, least / len(shards), largest / len(shards)))
        factor_of = factor_of * jnp.repeat(draws, shape[axis_at] // parts).reshape([-1 if axis == axis_at else 1 for axis in range(len(shape))])
    return factor_of


def normal_values(key, extent, deviation, reach, pieces=(), dtype=jnp.bfloat16):
    array = deviation * jax.random.normal(key, extent, jnp.float32)
    if pieces:
        array = array * block_scale(key, extent, pieces, -0.22, 0.18)
    return jnp.clip(array, -reach, reach).astype(dtype)


def setup_inputs(seed: int = 0) -> dict:
    key_list = jax.random.split(jax.random.key(seed), 4)
    residual = normal_values(key_list[0], (CHANNELS, NX, NCOL), 1.0, 6.0, ((0, 4), (1, 32)), jnp.float32)
    psf = normal_values(key_list[1], (CHANNELS, PATCH, PATCH), 0.3, 2.0, ((0, 4), (1, 32)), jnp.float32)
    positions = draw_positions(jax.random.fold_in(key_list[3], 71), 0)
    return {"residual": residual, "psf": psf, "positions": positions}


def reference(residual, psf, positions):
    half = PATCH // 2
    padded = jnp.pad(residual, ((0, 0), (half, half), (0, 0)))
    zero = jnp.int32(0)

    def step(k, image):
        row = positions[k, 0].astype(jnp.int32)
        col = positions[k, 1].astype(jnp.int32)
        value = lax.dynamic_slice(image, (zero, row + half, col), (CHANNELS, 1, 1)).reshape(CHANNELS)
        total = jnp.sum(value)
        amp = 0.25 * (value + total / CHANNELS)
        window = lax.dynamic_slice(image, (zero, row, col - half), (CHANNELS, PATCH, PATCH))
        window = window - amp[:, None, None] * psf
        return lax.dynamic_update_slice(image, window, (zero, row, col - half))
    padded = lax.fori_loop(0, STEPS, step, padded)
    image = padded[:, half:half + NX, :]
    summed = lax.optimization_barrier(jnp.sum(image, axis=0))
    mean_square = jnp.mean(summed * summed)
    return (image, summed * lax.rsqrt(mean_square + 1e-06))
```

```python
import functools

import jax
import jax.numpy as jnp
from jax import lax
from jax.experimental import pallas as pl
from jax.experimental.pallas import tpu as pltpu
from jax.sharding import Mesh
from jax.sharding import PartitionSpec as P

STEPS = 32
ROWS = ("rows_0", "rows_1", "rows_2")
CHAN_ROWS = ("chan", "rows_0", "rows_1", "rows_2")
LANES = 128
SUBLANES = 8
DEVICES = 128
NCHAN = 4
SLAB = 32
SHARD = 64
PATCH = 2048
HALF = PATCH // 2
NCOL = 16384
TALL = SLAB + SUBLANES
FOLD = LANES // STEPS


def floor_to(x, size):
    return pl.multiple_of(x - (x & (size - 1)), size)


def table_kernel(pos_ref, id_ref, psf_ref, res_ref, out_ref, tiles, wide, acc, sems):
    row_id = id_ref[0]
    first = row_id * SLAB
    lane = lax.broadcasted_iota(jnp.int32, (SUBLANES, LANES), 1)
    cell = lax.broadcasted_iota(jnp.int32, (SUBLANES, LANES), 0) * LANES + lane

    def tile_copy(k):
        local = jnp.clip(pos_ref[2 * k] - first, 0, SLAB - 1)
        src = res_ref.at[pl.ds(floor_to(local, SUBLANES), SUBLANES), pl.ds(floor_to(pos_ref[2 * k + 1], LANES), LANES)]
        return pltpu.make_async_copy(src, tiles.at[k], sems.at[k])

    def placed(tile, row, col, target, owned):
        turned = pltpu.roll(tile, (target - col) & (LANES - 1), 1)
        return cell == jnp.where(owned, (row & (SUBLANES - 1)) * LANES + target, -1), turned

    for k in range(STEPS):
        tile_copy(k).start()
    sums = [jnp.zeros((SUBLANES, LANES), jnp.float32) for _ in range(STEPS // FOLD)]
    for k in range(STEPS):
        base_row = pos_ref[2 * k] + HALF - row_id * SHARD
        base_col = pos_ref[2 * k + 1] + HALF
        for l in range(k):
            row = base_row - pos_ref[2 * l]
            col = base_col - pos_ref[2 * l + 1]
            owned = (row >= 0) & (row < SHARD) & (col >= 0) & (col < PATCH)
            row = jnp.clip(row, 0, SHARD - 1)
            col = jnp.clip(col, 0, PATCH - 1)
            tile = psf_ref[pl.ds(floor_to(row, SUBLANES), SUBLANES), pl.ds(floor_to(col, LANES), LANES)]
            here, turned = placed(tile, row, col, STEPS * (k % FOLD) + l, owned)
            sums[k // FOLD] = jnp.where(here, turned, sums[k // FOLD])
        if k % FOLD == FOLD - 1:
            wide[k // FOLD] = sums[k // FOLD]
    for k in range(STEPS):
        tile_copy(k).wait()
        local = pos_ref[2 * k] - first
        owned = (local >= 0) & (local < SLAB)
        here, turned = placed(tiles[k], jnp.clip(local, 0, SLAB - 1), pos_ref[2 * k + 1], STEPS * (k % FOLD) + k, owned)
        wide[k // FOLD] = jnp.where(here, turned, wide[k // FOLD])
    for g in range(STEPS // FOLD):
        acc[g : g + 1, :] = jnp.sum(wide[g], axis=0, keepdims=True)
    out_ref[...] = jnp.broadcast_to(acc[...][None], (DEVICES, SUBLANES, LANES))


def table(pos, ids, psf, residual):
    return pl.pallas_call(
        table_kernel,
        out_shape=jax.ShapeDtypeStruct((DEVICES, SUBLANES, LANES), jnp.float32),
        in_specs=[
            pl.BlockSpec(memory_space=pltpu.SMEM),
            pl.BlockSpec(memory_space=pltpu.SMEM),
            pl.BlockSpec(memory_space=pltpu.VMEM),
            pl.BlockSpec(memory_space=pl.ANY),
        ],
        out_specs=pl.BlockSpec(memory_space=pltpu.VMEM),
        scratch_shapes=[
            pltpu.VMEM((STEPS, SUBLANES, LANES), jnp.float32),
            pltpu.VMEM((SUBLANES, SUBLANES, LANES), jnp.float32),
            pltpu.VMEM((SUBLANES, LANES), jnp.float32),
            pltpu.SemaphoreType.DMA((STEPS,)),
        ],
        name="table",
    )(pos, ids, psf, residual)


def solve_kernel(id_ref, parts_ref, out_ref, rows):
    chan_id = id_ref[1]
    per_chan = DEVICES // NCHAN
    for c in range(NCHAN):
        summed = parts_ref[c * per_chan]
        for d in range(1, per_chan):
            summed = summed + parts_ref[c * per_chan + d]
        for g in range(SUBLANES):
            rows[g, c : c + 1, :] = summed[g : g + 1, :]
            rows[g, NCHAN + c : NCHAN + c + 1, :] = jnp.zeros((1, LANES), jnp.float32)
    lane = lax.broadcasted_iota(jnp.int32, (SUBLANES, LANES), 1)
    sub = lax.broadcasted_iota(jnp.int32, (SUBLANES, LANES), 0)
    at = lane % STEPS
    group = lane // STEPS
    own = sub == chan_id
    amps = jnp.zeros((SUBLANES, LANES), jnp.float32)
    for k in range(STEPS):
        weights = jnp.where(at == k, -1.0, amps)
        products = jnp.where(group == k % FOLD, rows[k // FOLD] * weights, 0.0)
        value = -jnp.sum(products, axis=1, keepdims=True)
        total = jnp.sum(value, axis=0, keepdims=True)
        amp = jnp.broadcast_to(0.25 * (value + total / NCHAN), (SUBLANES, LANES))
        amps = jnp.where((at == k) & (sub < NCHAN), amp, amps)
        mine = jnp.sum(jnp.where(own, amp, 0.0), axis=0, keepdims=True)
        out_ref[k] = jnp.broadcast_to(mine, (SUBLANES, LANES))


def solve(ids, parts):
    return pl.pallas_call(
        solve_kernel,
        out_shape=jax.ShapeDtypeStruct((STEPS, SUBLANES, LANES), jnp.float32),
        in_specs=[pl.BlockSpec(memory_space=pltpu.SMEM), pl.BlockSpec(memory_space=pltpu.VMEM)],
        out_specs=pl.BlockSpec(memory_space=pltpu.VMEM),
        scratch_shapes=[pltpu.VMEM((SUBLANES, SUBLANES, LANES), jnp.float32)],
        name="solve",
    )(ids, parts)


def apply_kernel(pos_ref, id_ref, amps_ref, psf_ref, res_ref, out_ref, image, windows, sems, edge_sems):
    first = id_ref[0] * SLAB
    lane = lax.broadcasted_iota(jnp.int32, (SUBLANES, LANES), 1)
    sub = lax.broadcasted_iota(jnp.int32, (SUBLANES, LANES), 0)

    def start_row(k):
        start = first - pos_ref[2 * k] + HALF
        return start, pl.multiple_of(jnp.minimum(start - (start & (SUBLANES - 1)), PATCH - TALL), SUBLANES)

    def window_copy(k):
        return pltpu.make_async_copy(psf_ref.at[pl.ds(start_row(k)[1], TALL), :], windows.at[k], sems.at[k])

    load = pltpu.make_async_copy(res_ref, image.at[:, pl.ds(0, NCOL)], edge_sems.at[0])
    load.start()
    lax.fori_loop(0, STEPS, lambda k, _: (window_copy(k).start(), 0)[1], 0)
    load.wait()

    def peak(k, _):
        window_copy(k).wait()
        start, aligned = start_row(k)
        off = start - aligned
        left = pos_ref[2 * k + 1] - HALF
        shift = left & (LANES - 1)
        base = left - shift
        amp = amps_ref[k]
        carried = lane < shift
        upper = sub < SUBLANES - off
        groups = TALL // SUBLANES
        before = [jnp.zeros((SUBLANES, LANES), jnp.float32)] * groups
        for t in range(PATCH // LANES + 1):
            if t < PATCH // LANES:
                turned = [
                    pltpu.roll(windows[k, pl.ds(g * SUBLANES, SUBLANES), pl.ds(t * LANES, LANES)], shift, 1)
                    for g in range(groups)
                ]
            else:
                turned = [jnp.zeros((SUBLANES, LANES), jnp.float32)] * groups
            joined = [pltpu.roll(jnp.where(carried, b, n), (SUBLANES - off) & (SUBLANES - 1), 0) for b, n in zip(before, turned)]
            cols = pl.ds(pl.multiple_of(base + t * LANES, LANES), LANES)
            for g in range(SLAB // SUBLANES):
                rows = pl.ds(g * SUBLANES, SUBLANES)
                image[rows, cols] = image[rows, cols] - amp * jnp.where(upper, joined[g], joined[g + 1])
            before = turned
        return 0

    lax.fori_loop(0, STEPS, peak, 0)
    store = pltpu.make_async_copy(image.at[:, pl.ds(0, NCOL)], out_ref, edge_sems.at[1])
    store.start()
    store.wait()


def apply(pos, ids, amps, psf, residual):
    return pl.pallas_call(
        apply_kernel,
        out_shape=jax.ShapeDtypeStruct((SLAB, NCOL), jnp.float32),
        in_specs=[
            pl.BlockSpec(memory_space=pltpu.SMEM),
            pl.BlockSpec(memory_space=pltpu.SMEM),
            pl.BlockSpec(memory_space=pltpu.VMEM),
            pl.BlockSpec(memory_space=pl.ANY),
            pl.BlockSpec(memory_space=pl.ANY),
        ],
        out_specs=pl.BlockSpec(memory_space=pl.ANY),
        scratch_shapes=[
            pltpu.VMEM((SLAB, NCOL + LANES), jnp.float32),
            pltpu.VMEM((STEPS, TALL, PATCH), jnp.float32),
            pltpu.SemaphoreType.DMA((STEPS,)),
            pltpu.SemaphoreType.DMA((2,)),
        ],
        compiler_params=pltpu.CompilerParams(vmem_limit_bytes=32 << 20),
        name="apply",
    )(pos, ids, amps, psf, residual)


def on_device(residual, psf, positions):
    chan_id = lax.axis_index("chan")
    row_id = lax.axis_index(ROWS)
    nrows = lax.axis_size(ROWS)
    slab, ncols = residual.shape[1:]
    ids = jnp.stack([row_id, chan_id]).astype(jnp.int32)
    pos = positions.reshape(-1)
    full_psf = lax.all_gather(psf[0], ROWS, axis=0, tiled=True)
    parts = table(pos, ids, psf[0], residual[0])
    parts = lax.all_to_all(parts, CHAN_ROWS, 0, 0, tiled=True)
    amps = solve(ids, parts)
    image = apply(pos, ids, amps, full_psf, residual[0])
    summed = lax.psum_scatter(image, "chan", scatter_dimension=1, tiled=True)
    square = jnp.broadcast_to(jnp.sum(summed * summed), (DEVICES, 1, LANES))
    total = jnp.sum(lax.all_to_all(square, CHAN_ROWS, 0, 0, tiled=True)[:, 0, 0])
    count = slab * nrows * ncols
    normalized = summed * lax.rsqrt(total / count + 1e-06)
    return (image[None], normalized)


def solution(mesh):
    finer = Mesh(
        mesh.devices.reshape(mesh.shape["chan"], 4, 4, 2), ("chan", "rows_0", "rows_1", "rows_2")
    )
    return jax.shard_map(
        on_device,
        mesh=finer,
        in_specs=(P("chan", ROWS, None), P("chan", ROWS, None), P()),
        out_specs=(P("chan", ROWS, None), P(ROWS, "chan")),
        check_vma=False,
    )
```

```python
import functools

import jax
import jax.numpy as jnp
from jax import lax
from jax.experimental import pallas as pl
from jax.experimental.pallas import tpu as pltpu
from jax.sharding import Mesh
from jax.sharding import PartitionSpec as P

STEPS = 32
ROWS = ("rows_0", "rows_1", "rows_2")
CHAN_ROWS = ("chan", "rows_0", "rows_1", "rows_2")
LANES = 128
SUBLANES = 8
DEVICES = 128
NCHAN = 4
SLAB = 32
SHARD = 64
PATCH = 2048
HALF = PATCH // 2
NCOL = 16384
TALL = SLAB + SUBLANES
FOLD = LANES // STEPS
QUARTER = NCOL // NCHAN
PIECES = (
    (0, 0, 32),
    (1, 0, 16),
    (1, 16, 16),
    (2, 0, 16),
    (2, 16, 16),
    (3, 0, 16),
    (3, 16, 16),
)


def floor_to(x, size):
    return pl.multiple_of(x - (x & (size - 1)), size)


def table_kernel(pos_ref, id_ref, psf_ref, res_ref, out_ref, tiles, wide, acc, sems):
    row_id = id_ref[0]
    first = row_id * SLAB
    lane = lax.broadcasted_iota(jnp.int32, (SUBLANES, LANES), 1)
    cell = lax.broadcasted_iota(jnp.int32, (SUBLANES, LANES), 0) * LANES + lane

    def tile_copy(k):
        local = jnp.clip(pos_ref[2 * k] - first, 0, SLAB - 1)
        src = res_ref.at[pl.ds(floor_to(local, SUBLANES), SUBLANES), pl.ds(floor_to(pos_ref[2 * k + 1], LANES), LANES)]
        return pltpu.make_async_copy(src, tiles.at[k], sems.at[k])

    def placed(tile, row, col, target, owned):
        turned = pltpu.roll(tile, (target - col) & (LANES - 1), 1)
        return cell == jnp.where(owned, (row & (SUBLANES - 1)) * LANES + target, -1), turned

    for k in range(STEPS):
        tile_copy(k).start()
    sums = [jnp.zeros((SUBLANES, LANES), jnp.float32) for _ in range(STEPS // FOLD)]
    for k in range(STEPS):
        base_row = pos_ref[2 * k] + HALF - row_id * SHARD
        base_col = pos_ref[2 * k + 1] + HALF
        for l in range(k):
            row = base_row - pos_ref[2 * l]
            col = base_col - pos_ref[2 * l + 1]
            owned = (row >= 0) & (row < SHARD) & (col >= 0) & (col < PATCH)
            row = jnp.clip(row, 0, SHARD - 1)
            col = jnp.clip(col, 0, PATCH - 1)
            tile = psf_ref[pl.ds(floor_to(row, SUBLANES), SUBLANES), pl.ds(floor_to(col, LANES), LANES)]
            here, turned = placed(tile, row, col, STEPS * (k % FOLD) + l, owned)
            sums[k // FOLD] = jnp.where(here, turned, sums[k // FOLD])
        if k % FOLD == FOLD - 1:
            wide[k // FOLD] = sums[k // FOLD]
    for k in range(STEPS):
        tile_copy(k).wait()
        local = pos_ref[2 * k] - first
        owned = (local >= 0) & (local < SLAB)
        here, turned = placed(tiles[k], jnp.clip(local, 0, SLAB - 1), pos_ref[2 * k + 1], STEPS * (k % FOLD) + k, owned)
        wide[k // FOLD] = jnp.where(here, turned, wide[k // FOLD])
    for g in range(STEPS // FOLD):
        acc[g : g + 1, :] = jnp.sum(wide[g], axis=0, keepdims=True)
    out_ref[...] = jnp.broadcast_to(acc[...][None], (DEVICES, SUBLANES, LANES))


def table(pos, ids, psf, residual):
    return pl.pallas_call(
        table_kernel,
        out_shape=jax.ShapeDtypeStruct((DEVICES, SUBLANES, LANES), jnp.float32),
        in_specs=[
            pl.BlockSpec(memory_space=pltpu.SMEM),
            pl.BlockSpec(memory_space=pltpu.SMEM),
            pl.BlockSpec(memory_space=pltpu.VMEM),
            pl.BlockSpec(memory_space=pl.ANY),
        ],
        out_specs=pl.BlockSpec(memory_space=pltpu.VMEM),
        scratch_shapes=[
            pltpu.VMEM((STEPS, SUBLANES, LANES), jnp.float32),
            pltpu.VMEM((SUBLANES, SUBLANES, LANES), jnp.float32),
            pltpu.VMEM((SUBLANES, LANES), jnp.float32),
            pltpu.SemaphoreType.DMA((STEPS,)),
        ],
        name="table",
    )(pos, ids, psf, residual)


def solve_kernel(id_ref, parts_ref, out_ref, rows):
    chan_id = id_ref[1]
    per_chan = DEVICES // NCHAN
    for c in range(NCHAN):
        summed = parts_ref[c * per_chan]
        for d in range(1, per_chan):
            summed = summed + parts_ref[c * per_chan + d]
        for g in range(SUBLANES):
            rows[g, c : c + 1, :] = summed[g : g + 1, :]
            rows[g, NCHAN + c : NCHAN + c + 1, :] = jnp.zeros((1, LANES), jnp.float32)
    lane = lax.broadcasted_iota(jnp.int32, (SUBLANES, LANES), 1)
    sub = lax.broadcasted_iota(jnp.int32, (SUBLANES, LANES), 0)
    at = lane % STEPS
    group = lane // STEPS
    own = sub == chan_id
    amps = jnp.zeros((SUBLANES, LANES), jnp.float32)
    for k in range(STEPS):
        weights = jnp.where(at == k, -1.0, amps)
        products = jnp.where(group == k % FOLD, rows[k // FOLD] * weights, 0.0)
        value = -jnp.sum(products, axis=1, keepdims=True)
        total = jnp.sum(value, axis=0, keepdims=True)
        amp = jnp.broadcast_to(0.25 * (value + total / NCHAN), (SUBLANES, LANES))
        amps = jnp.where((at == k) & (sub < NCHAN), amp, amps)
        mine = jnp.sum(jnp.where(own, amp, 0.0), axis=0, keepdims=True)
        out_ref[k] = jnp.broadcast_to(mine, (SUBLANES, LANES))


def solve(ids, parts):
    return pl.pallas_call(
        solve_kernel,
        out_shape=jax.ShapeDtypeStruct((STEPS, SUBLANES, LANES), jnp.float32),
        in_specs=[pl.BlockSpec(memory_space=pltpu.SMEM), pl.BlockSpec(memory_space=pltpu.VMEM)],
        out_specs=pl.BlockSpec(memory_space=pltpu.VMEM),
        scratch_shapes=[pltpu.VMEM((SUBLANES, SUBLANES, LANES), jnp.float32)],
        name="solve",
    )(ids, parts)


def apply_kernel(pos_ref, id_ref, amps_ref, psf_ref, res_ref, out_ref, *rest):
    *piece_refs, image, windows, sems, edge_sems = rest
    first = id_ref[0] * SLAB
    lane = lax.broadcasted_iota(jnp.int32, (SUBLANES, LANES), 1)
    sub = lax.broadcasted_iota(jnp.int32, (SUBLANES, LANES), 0)

    def start_row(k):
        start = first - pos_ref[2 * k] + HALF
        return start, pl.multiple_of(jnp.minimum(start - (start & (SUBLANES - 1)), PATCH - TALL), SUBLANES)

    def window_copy(k):
        return pltpu.make_async_copy(psf_ref.at[pl.ds(start_row(k)[1], TALL), :], windows.at[k], sems.at[k])

    load = pltpu.make_async_copy(res_ref, image.at[:, pl.ds(0, NCOL)], edge_sems.at[0])
    load.start()
    lax.fori_loop(0, STEPS, lambda k, _: (window_copy(k).start(), 0)[1], 0)
    load.wait()

    def peak(k, _):
        window_copy(k).wait()
        start, aligned = start_row(k)
        off = start - aligned
        left = pos_ref[2 * k + 1] - HALF
        shift = left & (LANES - 1)
        base = left - shift
        amp = amps_ref[k]
        carried = lane < shift
        upper = sub < SUBLANES - off
        groups = TALL // SUBLANES
        before = [jnp.zeros((SUBLANES, LANES), jnp.float32)] * groups
        for t in range(PATCH // LANES + 1):
            if t < PATCH // LANES:
                turned = [
                    pltpu.roll(windows[k, pl.ds(g * SUBLANES, SUBLANES), pl.ds(t * LANES, LANES)], shift, 1)
                    for g in range(groups)
                ]
            else:
                turned = [jnp.zeros((SUBLANES, LANES), jnp.float32)] * groups
            joined = [pltpu.roll(jnp.where(carried, b, n), (SUBLANES - off) & (SUBLANES - 1), 0) for b, n in zip(before, turned)]
            cols = pl.ds(pl.multiple_of(base + t * LANES, LANES), LANES)
            for g in range(SLAB // SUBLANES):
                rows = pl.ds(g * SUBLANES, SUBLANES)
                image[rows, cols] = image[rows, cols] - amp * jnp.where(upper, joined[g], joined[g + 1])
            before = turned
        return 0

    lax.fori_loop(0, STEPS, peak, 0)
    copies = [pltpu.make_async_copy(image.at[:, pl.ds(0, NCOL)], out_ref, edge_sems.at[0])]
    for n, ((ahead, top, tall), piece) in enumerate(zip(PIECES, piece_refs)):
        col = pl.multiple_of(((id_ref[1] + ahead) & (NCHAN - 1)) * QUARTER, QUARTER)
        src = image.at[pl.ds(top, tall), pl.ds(col, QUARTER)]
        copies.append(pltpu.make_async_copy(src, piece, edge_sems.at[n + 1]))
    for copy in reversed(copies):
        copy.start()
    for copy in copies:
        copy.wait()


def apply(pos, ids, amps, psf, residual):
    hbm = pl.BlockSpec(memory_space=pltpu.HBM)
    return pl.pallas_call(
        apply_kernel,
        out_shape=[
            jax.ShapeDtypeStruct((SLAB, NCOL), jnp.float32),
            *(jax.ShapeDtypeStruct((tall, QUARTER), jnp.float32) for _, _, tall in PIECES),
        ],
        in_specs=[
            pl.BlockSpec(memory_space=pltpu.SMEM),
            pl.BlockSpec(memory_space=pltpu.SMEM),
            pl.BlockSpec(memory_space=pltpu.VMEM),
            hbm,
            hbm,
        ],
        out_specs=[hbm] + [pl.BlockSpec(memory_space=pl.ANY)] * len(PIECES),
        scratch_shapes=[
            pltpu.VMEM((SLAB, NCOL + LANES), jnp.float32),
            pltpu.VMEM((STEPS, TALL, PATCH), jnp.float32),
            pltpu.SemaphoreType.DMA((STEPS,)),
            pltpu.SemaphoreType.DMA((len(PIECES) + 1,)),
        ],
        compiler_params=pltpu.CompilerParams(vmem_limit_bytes=52 << 20),
        name="apply",
    )(pos, ids, amps, psf, residual)


def channel_sum(pieces):
    mine, right_top, right_low, far_top, far_low, left_top, left_low = pieces

    def shift(x, by):
        return lax.ppermute(x, "chan", [(i, (i + by) % NCHAN) for i in range(NCHAN)])

    far_top, far_low = shift(far_top, 1), shift(far_low, 3)
    from_left_low, from_right_top = shift(right_low, 1), shift(left_top, 3)
    from_left_top, from_right_low = shift(right_top + far_top, 1), shift(left_low + far_low, 3)
    return mine + jnp.concatenate([from_left_top + from_right_top, from_left_low + from_right_low], 0)


def on_device(residual, psf, positions):
    chan_id = lax.axis_index("chan")
    row_id = lax.axis_index(ROWS)
    nrows = lax.axis_size(ROWS)
    slab, ncols = residual.shape[1:]
    ids = jnp.stack([row_id, chan_id]).astype(jnp.int32)
    pos = positions.reshape(-1)
    full_psf = lax.all_gather(psf[0], ROWS, axis=0, tiled=True)
    parts = table(pos, ids, psf[0], residual[0])
    parts = lax.all_to_all(parts, CHAN_ROWS, 0, 0, tiled=True)
    amps = solve(ids, parts)
    image, *pieces = apply(pos, ids, amps, full_psf, residual[0])
    summed = channel_sum(pieces)
    square = jnp.broadcast_to(jnp.sum(summed * summed), (DEVICES, 1, LANES))
    total = jnp.sum(lax.all_to_all(square, CHAN_ROWS, 0, 0, tiled=True)[:, 0, 0])
    count = slab * nrows * ncols
    normalized = summed * lax.rsqrt(total / count + 1e-06)
    return (image[None], normalized)


def solution(mesh):
    finer = Mesh(
        mesh.devices.reshape(mesh.shape["chan"], 4, 4, 2), ("chan", "rows_0", "rows_1", "rows_2")
    )
    return jax.shard_map(
        on_device,
        mesh=finer,
        in_specs=(P("chan", ROWS, None), P("chan", ROWS, None), P()),
        out_specs=(P("chan", ROWS, None), P(ROWS, "chan")),
        check_vma=False,
    )
```

```python
import functools

import jax
import jax.numpy as jnp
from jax import lax
from jax.experimental import pallas as pl
from jax.experimental.pallas import tpu as pltpu
from jax.sharding import Mesh
from jax.sharding import PartitionSpec as P

STEPS = 32
ROWS = ("rows_0", "rows_1", "rows_2")
CHAN_ROWS = ("chan", "rows_0", "rows_1", "rows_2")
LANES = 128
SUBLANES = 8
DEVICES = 128
NCHAN = 4
SLAB = 32
SHARD = 64
PATCH = 2048
HALF = PATCH // 2
NCOL = 16384
TALL = SLAB + SUBLANES
FOLD = LANES // STEPS
QUARTER = NCOL // NCHAN
SLOTS = 10
EDGE = 32
PART_VMEM = 40 << 20
BLOCKS = (
    ("own", 0),
    ("own", 1),
    ("own", 2),
    ("own", 3),
    ("near", 0),
    ("near", 1),
    ("near", 3),
    ("near_outer", 2),
    ("near_inner", 2),
    ("far", 0),
    ("far", 1),
    ("far", 2),
    ("far", 3),
)
PIECES = (
    (0, 0, 32),
    (1, 0, 16),
    (1, 16, 16),
    (2, 0, 16),
    (2, 16, 16),
    (3, 0, 16),
    (3, 16, 16),
)


def place_of_rows():
    return lax.axis_index("rows_0") * 8 + lax.axis_index("rows_1") * 2 + lax.axis_index("rows_2")


def floor_to(x, size):
    return pl.multiple_of(x - (x & (size - 1)), size)


def table_kernel(pos_ref, psf_ref, res_ref, out_ref, tiles, wide, acc, sems):
    row_id = place_of_rows()
    first = row_id * SLAB
    lane = lax.broadcasted_iota(jnp.int32, (SUBLANES, LANES), 1)
    cell = lax.broadcasted_iota(jnp.int32, (SUBLANES, LANES), 0) * LANES + lane

    def tile_copy(k):
        local = (pos_ref[0, k] - first) & (SLAB - 1)
        src = res_ref.at[pl.ds(floor_to(local, SUBLANES), SUBLANES), pl.ds(floor_to(pos_ref[1, k], LANES), LANES)]
        return pltpu.make_async_copy(src, tiles.at[k], sems.at[k])

    def placed(tile, row, col, target, foreign):
        turned = pltpu.roll(tile, (target - col) & (LANES - 1), 1)
        code = (row & (SUBLANES - 1)) * LANES + target
        return cell == jnp.where(foreign == 0, code, -1), turned

    for k in range(STEPS):
        tile_copy(k).start()
    sums = [jnp.zeros((SUBLANES, LANES), jnp.float32) for _ in range(STEPS // FOLD)]
    for k in range(STEPS):
        base_row = pos_ref[0, k] + (HALF - row_id * SHARD)
        base_col = pos_ref[1, k] + HALF
        for l in range(k):
            row = base_row - pos_ref[0, l]
            col = base_col - pos_ref[1, l]
            foreign = (row >> 6) | (col >> 11)
            rows = pl.ds(pl.multiple_of(row & (SHARD - SUBLANES), SUBLANES), SUBLANES)
            cols = pl.ds(pl.multiple_of(col & (PATCH - LANES), LANES), LANES)
            here, turned = placed(psf_ref[rows, cols], row, col, STEPS * (k % FOLD) + l, foreign)
            sums[k // FOLD] = jnp.where(here, turned, sums[k // FOLD])
        if k % FOLD == FOLD - 1:
            wide[k // FOLD] = sums[k // FOLD]
    for k in range(STEPS):
        tile_copy(k).wait()
        local = pos_ref[0, k] - first
        here, turned = placed(tiles[k], local, pos_ref[1, k], STEPS * (k % FOLD) + k, local >> 5)
        wide[k // FOLD] = jnp.where(here, turned, wide[k // FOLD])
    for g in range(STEPS // FOLD):
        acc[g : g + 1, :] = jnp.sum(wide[g], axis=0, keepdims=True)
    out_ref[...] = jnp.broadcast_to(acc[...][None], (DEVICES, SUBLANES, LANES))


def table(pos, psf, residual):
    return pl.pallas_call(
        table_kernel,
        out_shape=jax.ShapeDtypeStruct((DEVICES, SUBLANES, LANES), jnp.float32),
        in_specs=[
            pl.BlockSpec(memory_space=pltpu.SMEM),
            pl.BlockSpec(memory_space=pltpu.VMEM),
            pl.BlockSpec(memory_space=pl.ANY),
        ],
        out_specs=pl.BlockSpec(memory_space=pltpu.VMEM),
        scratch_shapes=[
            pltpu.VMEM((STEPS, SUBLANES, LANES), jnp.float32),
            pltpu.VMEM((SUBLANES, SUBLANES, LANES), jnp.float32),
            pltpu.VMEM((SUBLANES, LANES), jnp.float32),
            pltpu.SemaphoreType.DMA((STEPS,)),
        ],
        name="table",
    )(pos, psf, residual)


def solve_kernel(parts_ref, out_ref, rows):
    chan_id = lax.axis_index("chan")
    per_chan = DEVICES // NCHAN
    for c in range(NCHAN):
        summed = parts_ref[c * per_chan]
        for d in range(1, per_chan):
            summed = summed + parts_ref[c * per_chan + d]
        for g in range(SUBLANES):
            rows[g, c : c + 1, :] = summed[g : g + 1, :]
            rows[g, NCHAN + c : NCHAN + c + 1, :] = jnp.zeros((1, LANES), jnp.float32)
    lane = lax.broadcasted_iota(jnp.int32, (SUBLANES, LANES), 1)
    sub = lax.broadcasted_iota(jnp.int32, (SUBLANES, LANES), 0)
    at = lane % STEPS
    group = lane // STEPS
    own = sub == chan_id
    amps = jnp.zeros((SUBLANES, LANES), jnp.float32)
    for k in range(STEPS):
        weights = jnp.where(at == k, -1.0, amps)
        products = jnp.where(group == k % FOLD, rows[k // FOLD] * weights, 0.0)
        value = -jnp.sum(products, axis=1, keepdims=True)
        total = jnp.sum(value, axis=0, keepdims=True)
        amp = jnp.broadcast_to(0.25 * (value + total / NCHAN), (SUBLANES, LANES))
        amps = jnp.where((at == k) & (sub < NCHAN), amp, amps)
        mine = jnp.sum(jnp.where(own, amp, 0.0), axis=0, keepdims=True)
        out_ref[k] = jnp.broadcast_to(mine, (SUBLANES, LANES))


def solve(parts):
    return pl.pallas_call(
        solve_kernel,
        out_shape=jax.ShapeDtypeStruct((STEPS, SUBLANES, LANES), jnp.float32),
        in_specs=[pl.BlockSpec(memory_space=pltpu.VMEM)],
        out_specs=pl.BlockSpec(memory_space=pltpu.VMEM),
        scratch_shapes=[pltpu.VMEM((SUBLANES, SUBLANES, LANES), jnp.float32)],
        name="solve",
    )(parts)


NEAR = (1, 2, 1, 2)
HALFWAY = (2, 0, 3, 1)


def place(z, y, c):
    return z * 8 + y * 2 + c


def needs(z, y, c, j):
    return 4 * z + y <= 2 * j + c <= 4 * z + y + 16


def near_held(z, y):
    return 4 * NEAR[z] + y


def halfway_held(z, y):
    return 4 * HALFWAY[z] + y if (y < 2) == (z % 2 == 0) else None


def turn(by, held):
    chips = [(z, y) for z in range(4) for y in range(4) if held(z, y) is not None]
    return [
        (place(z, y, c), place(z, (y + by) % 4, c))
        for z, y in chips
        for c in range(2)
        if needs(z, (y + by) % 4, c, held(z, y))
    ]


def climb(moves):
    return [(place(a, y, c), place(b, y, c)) for a, b in moves for y in range(4) for c in range(2)]


OUTER = climb([(1, 0), (2, 3)])
INNER = climb([(2, 1), (1, 2)])
ACROSS = [
    (place(HALFWAY[z], y, c), place(z, y, c))
    for z in range(4)
    for y in range(4)
    for c in range(2)
    if halfway_held(z, y) is not None
]


def permute(x, pairs):
    return lax.ppermute(x, ROWS, pairs)


def part_kernel(mine, pos_ref, amps_ref, *rest):
    n = len(BLOCKS)
    block_refs = rest[:n]
    res_ref, out_ref, image, patch, sems, edge_sems = rest[n:] if mine else (None, *rest[n:])
    z, y, c = (lax.axis_index(name) for name in ROWS)
    half = c if mine else 1 - c
    first = (4 * z + y) * SHARD + half * SLAB
    inner = (z == 1) | (z == 2)
    odd = z & 1
    own_slot = 2 * z
    near_slot = jnp.where(z == 0, 4, jnp.where(z == 1, 6, jnp.where(z == 2, 0, 2)))
    far_slot = jnp.where(odd == 0, 8, -2)
    lane = lax.broadcasted_iota(jnp.int32, (SUBLANES, LANES), 1)
    sub = lax.broadcasted_iota(jnp.int32, (SUBLANES, LANES), 0)

    def block_copy(i):
        kind, by = BLOCKS[i]
        source = (y - by) & 3
        if kind == "own":
            slot, held = own_slot + source, None
        elif kind == "far":
            slot, held = far_slot + source, (source >> 1) == odd
        else:
            slot = near_slot + source
            held = None if kind == "near" else inner == (kind == "near_inner")
        slot = jnp.clip(slot, 0, SLOTS - 1)
        rows = pl.ds(pl.multiple_of(EDGE + slot * SHARD, SUBLANES), SHARD)
        copy = pltpu.make_async_copy(block_refs[i], patch.at[rows, :], sems.at[i])
        return copy, held

    def each_block(act):
        for i in range(n):
            copy, held = block_copy(i)
            if held is None:
                act(copy)
            else:
                pl.when(held)(functools.partial(act, copy))

    each_block(lambda copy: copy.start())
    if mine:
        load = pltpu.make_async_copy(res_ref, image.at[:, pl.ds(0, NCOL)], edge_sems.at[0])
        load.start()
    else:
        image[...] = jnp.zeros(image.shape, jnp.float32)
    patch[pl.ds(0, EDGE), :] = jnp.zeros((EDGE, PATCH), jnp.float32)
    patch[pl.ds(EDGE + SLOTS * SHARD, EDGE), :] = jnp.zeros((EDGE, PATCH), jnp.float32)
    each_block(lambda copy: copy.wait())
    if mine:
        load.wait()

    def peak(k, _):
        start = first - pos_ref[0, k] + HALF
        other = ((start >> 6) ^ c) & 1
        skew = (start & (SHARD - 1)) - other * SHARD

        @pl.when(skew > -SLAB)
        def _():
            slot = (((start >> 6) + other) >> 1) - 2 * z
            row = EDGE + slot * SHARD + skew
            off = row & (SUBLANES - 1)
            row = row - off
            left = pos_ref[1, k] - HALF
            shift = left & (LANES - 1)
            base = left - shift
            amp = amps_ref[k]
            carried = lane < shift
            upper = sub < SUBLANES - off
            groups = TALL // SUBLANES
            within = [sub + (g * SUBLANES + skew) for g in range(SLAB // SUBLANES)]
            scales = [jnp.where((at >= 0) & (at < SHARD), amp, 0.0) for at in within]
            before = [jnp.zeros((SUBLANES, LANES), jnp.float32)] * groups
            for t in range(PATCH // LANES + 1):
                if t < PATCH // LANES:
                    turned = []
                    for g in range(groups):
                        rows = pl.ds(pl.multiple_of(row + g * SUBLANES, SUBLANES), SUBLANES)
                        turned.append(pltpu.roll(patch[rows, pl.ds(t * LANES, LANES)], shift, 1))
                else:
                    turned = [jnp.zeros((SUBLANES, LANES), jnp.float32)] * groups
                back = (SUBLANES - off) & (SUBLANES - 1)
                joined = [pltpu.roll(jnp.where(carried, b, n), back, 0) for b, n in zip(before, turned)]
                cols = pl.ds(pl.multiple_of(base + t * LANES, LANES), LANES)
                for g in range(SLAB // SUBLANES):
                    rows = pl.ds(g * SUBLANES, SUBLANES)
                    value = jnp.where(upper, joined[g], joined[g + 1])
                    image[rows, cols] = image[rows, cols] - scales[g] * value
                before = turned

        return 0

    lax.fori_loop(0, STEPS, peak, 0)
    store = pltpu.make_async_copy(image.at[:, pl.ds(0, NCOL)], out_ref, edge_sems.at[1])
    store.start()
    store.wait()


def part(mine, pos, amps, blocks, residual):
    anywhere = pl.BlockSpec(memory_space=pl.ANY)
    operands = (*blocks, residual) if mine else blocks
    return pl.pallas_call(
        functools.partial(part_kernel, mine),
        out_shape=jax.ShapeDtypeStruct((SLAB, NCOL), jnp.float32),
        in_specs=[pl.BlockSpec(memory_space=pltpu.SMEM), pl.BlockSpec(memory_space=pltpu.VMEM)] + [anywhere] * len(operands),
        out_specs=anywhere,
        scratch_shapes=[
            pltpu.VMEM((SLAB, NCOL + LANES), jnp.float32),
            pltpu.VMEM((2 * EDGE + SLOTS * SHARD, PATCH), jnp.float32),
            pltpu.SemaphoreType.DMA((len(BLOCKS),)),
            pltpu.SemaphoreType.DMA((2,)),
        ],
        compiler_params=pltpu.CompilerParams(vmem_limit_bytes=PART_VMEM),
        name="mine" if mine else "yours",
    )(pos, amps, *operands)


def join_kernel(mine_ref, other_ref, out_ref, *piece_refs):
    chan_id = lax.axis_index("chan")
    for n in range(NCHAN):
        cols = pl.ds(n * QUARTER, QUARTER)
        out_ref[:, cols] = mine_ref[:, cols] + other_ref[:, cols]
    for (ahead, top, tall), piece in zip(PIECES, piece_refs):
        col = pl.multiple_of(((chan_id + ahead) & (NCHAN - 1)) * QUARTER, QUARTER)
        piece[...] = out_ref[pl.ds(top, tall), pl.ds(col, QUARTER)]


def join(mine, other):
    vmem = pl.BlockSpec(memory_space=pltpu.VMEM)
    return pl.pallas_call(
        join_kernel,
        out_shape=[
            jax.ShapeDtypeStruct((SLAB, NCOL), jnp.float32),
            *(jax.ShapeDtypeStruct((tall, QUARTER), jnp.float32) for _, _, tall in PIECES),
        ],
        in_specs=[vmem, vmem],
        out_specs=[vmem] * (len(PIECES) + 1),
        name="join",
    )(mine, other)


def channel_sum(pieces):
    mine, right_top, right_low, far_top, far_low, left_top, left_low = pieces

    def shift(x, by):
        return lax.ppermute(x, "chan", [(i, (i + by) % NCHAN) for i in range(NCHAN)])

    far_top, far_low = shift(far_top, 1), shift(far_low, 3)
    from_left_low, from_right_top = shift(right_low, 1), shift(left_top, 3)
    from_left_top, from_right_low = shift(right_top + far_top, 1), shift(left_low + far_low, 3)
    return mine + jnp.concatenate([from_left_top + from_right_top, from_left_low + from_right_low], 0)


def on_device(residual, psf, positions):
    nrows = lax.axis_size(ROWS)
    slab, ncols = residual.shape[1:]
    z = lax.axis_index("rows_0")
    outer = (z == 0) | (z == 3)
    pos = positions.T
    own = psf[0]
    to_outer, to_inner = permute(own, OUTER), permute(own, INNER)
    own1, own3, own2 = (permute(own, turn(by, lambda z, y: 4 * z + y)) for by in (1, 3, 2))
    far = permute(own, ACROSS)
    parts = table(pos, own, residual[0])
    parts = lax.all_to_all(parts, CHAN_ROWS, 0, 0, tiled=True)
    to_outer, to_inner, far, own2, parts = lax.optimization_barrier((to_outer, to_inner, far, own2, parts))
    near = jnp.where(outer, to_outer, to_inner)
    near1, near3 = (permute(near, turn(by, near_held)) for by in (1, 3))
    far1, far2, far3 = (permute(far, turn(by, halfway_held)) for by in (1, 2, 3))
    near2_outer, near2_inner = permute(own2, OUTER), permute(own2, INNER)
    amps = solve(parts)
    blocks = (own, own1, own2, own3, near, near1, near3, near2_outer, near2_inner, far, far1, far2, far3)
    yours = part(False, pos, amps, blocks, residual[0])
    other = lax.ppermute(yours, "rows_2", [(0, 1), (1, 0)])
    mine = part(True, pos, amps, blocks, residual[0])
    image, *pieces = join(mine, other)
    summed = channel_sum(pieces)
    square = jnp.broadcast_to(jnp.sum(summed * summed), (DEVICES, 1, LANES))
    total = jnp.sum(lax.all_to_all(square, CHAN_ROWS, 0, 0, tiled=True)[:, 0, 0])
    count = slab * nrows * ncols
    normalized = summed * lax.rsqrt(total / count + 1e-06)
    return (image[None], normalized)


def solution(mesh):
    finer = Mesh(
        mesh.devices.reshape(mesh.shape["chan"], 4, 4, 2), ("chan", "rows_0", "rows_1", "rows_2")
    )
    return jax.shard_map(
        on_device,
        mesh=finer,
        in_specs=(P("chan", ROWS, None), P("chan", ROWS, None), P()),
        out_specs=(P("chan", ROWS, None), P(ROWS, "chan")),
        check_vma=False,
    )
```

```python
import functools

import jax
import jax.numpy as jnp
from jax import lax
from jax.experimental import pallas as pl
from jax.experimental.pallas import tpu as pltpu
from jax.sharding import Mesh
from jax.sharding import PartitionSpec as P


STEPS = 32
ROWS = ("rows_0", "rows_1", "rows_2")
CHAN_ROWS = ("chan", "rows_0", "rows_1", "rows_2")
LANES = 128
SUBLANES = 8
DEVICES = 128
NCHAN = 4
SLAB = 32
SHARD = 64
PATCH = 2048
HALF = PATCH // 2
NCOL = 16384
TALL = SLAB + SUBLANES
FOLD = LANES // STEPS
QUARTER = NCOL // NCHAN
SLOTS = 10
EDGE = 32
PART_VMEM = 40 << 20
JOIN_VMEM = 12 << 20
EARLY = (("own", 0), ("own", 1), ("own", 2), ("own", 3), ("near", 0), ("near", 1), ("near", 3))
LATE = (("near_outer", 2), ("near_inner", 2), ("far", 0), ("far", 1), ("far", 2), ("far", 3))
PIECES = (
    (0, 0, 32),
    (1, 0, 16),
    (1, 16, 16),
    (2, 0, 16),
    (2, 16, 16),
    (3, 0, 16),
    (3, 16, 16),
)


def place_of_rows():
    return lax.axis_index("rows_0") * 8 + lax.axis_index("rows_1") * 2 + lax.axis_index("rows_2")


def floor_to(x, size):
    return pl.multiple_of(x - (x & (size - 1)), size)


def table_kernel(pos_ref, psf_ref, res_ref, out_ref, tiles, wide, acc, sems):
    row_id = place_of_rows()
    first = row_id * SLAB
    lane = lax.broadcasted_iota(jnp.int32, (SUBLANES, LANES), 1)
    cell = lax.broadcasted_iota(jnp.int32, (SUBLANES, LANES), 0) * LANES + lane

    def tile_copy(k):
        local = (pos_ref[0, k] - first) & (SLAB - 1)
        src = res_ref.at[pl.ds(floor_to(local, SUBLANES), SUBLANES), pl.ds(floor_to(pos_ref[1, k], LANES), LANES)]
        return pltpu.make_async_copy(src, tiles.at[k], sems.at[k])

    def placed(tile, row, col, target, foreign):
        turned = pltpu.roll(tile, (target - col) & (LANES - 1), 1)
        code = (row & (SUBLANES - 1)) * LANES + target
        return cell == jnp.where(foreign == 0, code, -1), turned

    for k in range(STEPS):
        tile_copy(k).start()
    sums = [jnp.zeros((SUBLANES, LANES), jnp.float32) for _ in range(STEPS // FOLD)]
    for k in range(STEPS):
        base_row = pos_ref[0, k] + (HALF - row_id * SHARD)
        base_col = pos_ref[1, k] + HALF
        for l in range(k):
            row = base_row - pos_ref[0, l]
            col = base_col - pos_ref[1, l]
            foreign = (row >> 6) | (col >> 11)
            rows = pl.ds(pl.multiple_of(row & (SHARD - SUBLANES), SUBLANES), SUBLANES)
            cols = pl.ds(pl.multiple_of(col & (PATCH - LANES), LANES), LANES)
            here, turned = placed(psf_ref[rows, cols], row, col, STEPS * (k % FOLD) + l, foreign)
            sums[k // FOLD] = jnp.where(here, turned, sums[k // FOLD])
        if k % FOLD == FOLD - 1:
            wide[k // FOLD] = sums[k // FOLD]
    for k in range(STEPS):
        tile_copy(k).wait()
        local = pos_ref[0, k] - first
        here, turned = placed(tiles[k], local, pos_ref[1, k], STEPS * (k % FOLD) + k, local >> 5)
        wide[k // FOLD] = jnp.where(here, turned, wide[k // FOLD])
    for g in range(STEPS // FOLD):
        acc[g : g + 1, :] = jnp.sum(wide[g], axis=0, keepdims=True)
    out_ref[...] = jnp.broadcast_to(acc[...][None], (DEVICES, SUBLANES, LANES))


def table(pos, psf, residual):
    return pl.pallas_call(
        table_kernel,
        out_shape=jax.ShapeDtypeStruct((DEVICES, SUBLANES, LANES), jnp.float32),
        in_specs=[
            pl.BlockSpec(memory_space=pltpu.SMEM),
            pl.BlockSpec(memory_space=pltpu.VMEM),
            pl.BlockSpec(memory_space=pl.ANY),
        ],
        out_specs=pl.BlockSpec(memory_space=pltpu.VMEM),
        scratch_shapes=[
            pltpu.VMEM((STEPS, SUBLANES, LANES), jnp.float32),
            pltpu.VMEM((SUBLANES, SUBLANES, LANES), jnp.float32),
            pltpu.VMEM((SUBLANES, LANES), jnp.float32),
            pltpu.SemaphoreType.DMA((STEPS,)),
        ],
        name="table",
    )(pos, psf, residual)


def solve_kernel(parts_ref, out_ref, rows):
    chan_id = lax.axis_index("chan")
    per_chan = DEVICES // NCHAN
    for c in range(NCHAN):
        summed = parts_ref[c * per_chan]
        for d in range(1, per_chan):
            summed = summed + parts_ref[c * per_chan + d]
        for g in range(SUBLANES):
            rows[g, c : c + 1, :] = summed[g : g + 1, :]
            rows[g, NCHAN + c : NCHAN + c + 1, :] = jnp.zeros((1, LANES), jnp.float32)
    lane = lax.broadcasted_iota(jnp.int32, (SUBLANES, LANES), 1)
    sub = lax.broadcasted_iota(jnp.int32, (SUBLANES, LANES), 0)
    at = lane % STEPS
    group = lane // STEPS
    own = sub == chan_id
    amps = jnp.zeros((SUBLANES, LANES), jnp.float32)
    for k in range(STEPS):
        weights = jnp.where(at == k, -1.0, amps)
        products = jnp.where(group == k % FOLD, rows[k // FOLD] * weights, 0.0)
        value = -jnp.sum(products, axis=1, keepdims=True)
        total = jnp.sum(value, axis=0, keepdims=True)
        amp = jnp.broadcast_to(0.25 * (value + total / NCHAN), (SUBLANES, LANES))
        amps = jnp.where((at == k) & (sub < NCHAN), amp, amps)
        mine = jnp.sum(jnp.where(own, amp, 0.0), axis=0, keepdims=True)
        out_ref[k] = jnp.broadcast_to(mine, (SUBLANES, LANES))


def solve(parts):
    return pl.pallas_call(
        solve_kernel,
        out_shape=jax.ShapeDtypeStruct((STEPS, SUBLANES, LANES), jnp.float32),
        in_specs=[pl.BlockSpec(memory_space=pltpu.VMEM)],
        out_specs=pl.BlockSpec(memory_space=pltpu.VMEM),
        scratch_shapes=[pltpu.VMEM((SUBLANES, SUBLANES, LANES), jnp.float32)],
        name="solve",
    )(parts)


NEAR = (1, 2, 1, 2)
HALFWAY = (2, 0, 3, 1)


def place(z, y, c):
    return z * 8 + y * 2 + c


def needs(z, y, c, j):
    return 4 * z + y <= 2 * j + c <= 4 * z + y + 16


def near_held(z, y):
    return 4 * NEAR[z] + y


def halfway_held(z, y):
    return 4 * HALFWAY[z] + y if (y < 2) == (z % 2 == 0) else None


def turn(by, held):
    chips = [(z, y) for z in range(4) for y in range(4) if held(z, y) is not None]
    return [
        (place(z, y, c), place(z, (y + by) % 4, c))
        for z, y in chips
        for c in range(2)
        if needs(z, (y + by) % 4, c, held(z, y))
    ]


def climb(moves):
    return [(place(a, y, c), place(b, y, c)) for a, b in moves for y in range(4) for c in range(2)]


OUTER = climb([(1, 0), (2, 3)])
INNER = climb([(2, 1), (1, 2)])
ACROSS = [
    (place(HALFWAY[z], y, c), place(z, y, c))
    for z in range(4)
    for y in range(4)
    for c in range(2)
    if halfway_held(z, y) is not None
]


def permute(x, pairs):
    return lax.ppermute(x, ROWS, pairs)


def part_kernel(names, halves, late, from_residual, pos_ref, amps_ref, *rest):
    count = len(names)
    block_refs, rest = rest[:count], rest[count:]
    base_refs, rest = rest[: 1 if from_residual else len(halves)], rest[1 if from_residual else len(halves) :]
    out_refs, rest = rest[: len(halves)], rest[len(halves) :]
    images, (patch, sems, edge_sems) = rest[: len(halves)], rest[len(halves) :]
    z, y, c = (lax.axis_index(name) for name in ROWS)
    inner = (z == 1) | (z == 2)
    odd = z & 1
    near_slot = jnp.where(z == 0, 4, jnp.where(z == 1, 6, jnp.where(z == 2, 0, 2)))
    far_slot = jnp.where(odd == 0, 8, -2)
    lane = lax.broadcasted_iota(jnp.int32, (SUBLANES, LANES), 1)
    sub = lax.broadcasted_iota(jnp.int32, (SUBLANES, LANES), 0)

    def each_block(act):
        for i, (kind, by) in enumerate(names):
            source = (y - by) & 3
            if kind == "own":
                slot, held = 2 * z + source, None
            elif kind == "far":
                slot, held = far_slot + source, (source >> 1) == odd
            else:
                slot = near_slot + source
                held = None if kind == "near" else inner == (kind == "near_inner")
            slot = jnp.clip(slot, 0, SLOTS - 1)
            rows = pl.ds(pl.multiple_of(EDGE + slot * SHARD, SUBLANES), SHARD)
            copy = pltpu.make_async_copy(block_refs[i], patch.at[rows, :], sems.at[i])
            if held is None:
                act(copy)
            else:
                pl.when(held)(functools.partial(act, copy))

    each_block(lambda copy: copy.start())
    loads = []
    for n, image in enumerate(images):
        if from_residual and halves[n] == 1:
            image[...] = jnp.zeros(image.shape, jnp.float32)
        else:
            base = base_refs[0 if from_residual else n]
            loads.append(pltpu.make_async_copy(base, image.at[:, pl.ds(0, NCOL)], edge_sems.at[n]))
            loads[-1].start()
    each_block(lambda copy: copy.wait())
    for load in loads:
        load.wait()

    def peak(image, first, k):
        start = first - pos_ref[0, k] + HALF
        other = ((start >> 6) ^ c) & 1
        skew = (start & (SHARD - 1)) - other * SHARD
        slot = (((start >> 6) + other) >> 1) - 2 * z
        is_late = ((slot >> 1) == jnp.where(odd == 0, 4, 0)) | (slot == near_slot + ((y + 2) & 3))

        @pl.when((skew > -SLAB) & (is_late == late))
        def _():
            row = EDGE + slot * SHARD + skew
            off = row & (SUBLANES - 1)
            row = row - off
            left = pos_ref[1, k] - HALF
            shift = left & (LANES - 1)
            base = left - shift
            amp = amps_ref[k]
            carried = lane < shift
            upper = sub < SUBLANES - off
            groups = TALL // SUBLANES
            places = [sub + (g * SUBLANES + skew) for g in range(SLAB // SUBLANES)]
            within = [(at >= 0) & (at < SHARD) for at in places]
            before = [jnp.zeros((SUBLANES, LANES), jnp.float32)] * groups
            for t in range(PATCH // LANES + 1):
                if t < PATCH // LANES:
                    turned = []
                    for g in range(groups):
                        rows = pl.ds(pl.multiple_of(row + g * SUBLANES, SUBLANES), SUBLANES)
                        turned.append(pltpu.roll(patch[rows, pl.ds(t * LANES, LANES)], shift, 1))
                else:
                    turned = [jnp.zeros((SUBLANES, LANES), jnp.float32)] * groups
                back = (SUBLANES - off) & (SUBLANES - 1)
                joined = [pltpu.roll(jnp.where(carried, b, n), back, 0) for b, n in zip(before, turned)]
                cols = pl.ds(pl.multiple_of(base + t * LANES, LANES), LANES)
                for g in range(SLAB // SUBLANES):
                    rows = pl.ds(g * SUBLANES, SUBLANES)
                    value = jnp.where(within[g], jnp.where(upper, joined[g], joined[g + 1]), 0.0)
                    image[rows, cols] = image[rows, cols] - amp * value
                before = turned

    stores = []
    for n, image in enumerate(images):
        half = c if halves[n] == 0 else 1 - c
        first = (4 * z + y) * SHARD + half * SLAB
        lax.fori_loop(0, STEPS, lambda k, _, image=image, first=first: (peak(image, first, k), 0)[1], 0)
        stores.append(pltpu.make_async_copy(image.at[:, pl.ds(0, NCOL)], out_refs[n], edge_sems.at[n]))
        stores[-1].start()
    for store in stores:
        store.wait()


def part(names, halves, late, pos, amps, blocks, bases):
    anywhere = pl.BlockSpec(memory_space=pl.ANY)
    from_residual = not late
    return pl.pallas_call(
        functools.partial(part_kernel, names, halves, late, from_residual),
        out_shape=[jax.ShapeDtypeStruct((SLAB, NCOL), jnp.float32)] * len(halves),
        in_specs=[pl.BlockSpec(memory_space=pltpu.SMEM), pl.BlockSpec(memory_space=pltpu.VMEM)]
        + [anywhere] * (len(blocks) + len(bases)),
        out_specs=[anywhere] * len(halves),
        scratch_shapes=[pltpu.VMEM((SLAB, NCOL + LANES), jnp.float32)] * len(halves)
        + [
            pltpu.VMEM((2 * EDGE + SLOTS * SHARD, PATCH), jnp.float32),
            pltpu.SemaphoreType.DMA((len(names),)),
            pltpu.SemaphoreType.DMA((len(halves),)),
        ],
        compiler_params=pltpu.CompilerParams(vmem_limit_bytes=PART_VMEM),
    )(pos, amps, *blocks, *bases)


def join_kernel(mine_ref, other_ref, out_ref, *rest):
    piece_refs, (mine, other, sems, piece_sems) = rest[: len(PIECES)], rest[len(PIECES) :]
    chan_id = lax.axis_index("chan")

    def cols(ahead):
        return pl.ds(pl.multiple_of(((chan_id + ahead) & (NCHAN - 1)) * QUARTER, QUARTER), QUARTER)

    def load(ahead, n):
        src, dst = ((mine_ref, mine), (other_ref, other))[n]
        return pltpu.make_async_copy(src.at[:, cols(ahead)], dst.at[ahead], sems.at[n, ahead])

    order = (2, 1, 3, 0)
    for ahead in order:
        load(ahead, 0).start()
        load(ahead, 1).start()
    stores = []
    for ahead in order:
        load(ahead, 0).wait()
        load(ahead, 1).wait()
        mine[ahead] = mine[ahead] + other[ahead]
        stores.append(pltpu.make_async_copy(mine.at[ahead], out_ref.at[:, cols(ahead)], sems.at[2, ahead]))
        stores[-1].start()
        for i, (where, top, tall) in enumerate(PIECES):
            if where == ahead:
                src = mine.at[ahead, pl.ds(top, tall), :]
                stores.append(pltpu.make_async_copy(src, piece_refs[i], piece_sems.at[i]))
                stores[-1].start()
    for store in stores:
        store.wait()


def join(mine, other):
    anywhere = pl.BlockSpec(memory_space=pl.ANY)
    return pl.pallas_call(
        join_kernel,
        out_shape=[
            jax.ShapeDtypeStruct((SLAB, NCOL), jnp.float32),
            *(jax.ShapeDtypeStruct((tall, QUARTER), jnp.float32) for _, _, tall in PIECES),
        ],
        in_specs=[anywhere] * 2,
        out_specs=[anywhere] * (len(PIECES) + 1),
        scratch_shapes=[
            pltpu.VMEM((NCHAN, SLAB, QUARTER), jnp.float32),
            pltpu.VMEM((NCHAN, SLAB, QUARTER), jnp.float32),
            pltpu.SemaphoreType.DMA((3, NCHAN)),
            pltpu.SemaphoreType.DMA((len(PIECES),)),
        ],
        compiler_params=pltpu.CompilerParams(vmem_limit_bytes=JOIN_VMEM),
        name="join",
    )(mine, other)


def channel_sum(pieces):
    mine, right_top, right_low, far_top, far_low, left_top, left_low = pieces

    def shift(x, by):
        return lax.ppermute(x, "chan", [(i, (i + by) % NCHAN) for i in range(NCHAN)])

    far_top, far_low = shift(far_top, 1), shift(far_low, 3)
    from_left_low, from_right_top = shift(right_low, 1), shift(left_top, 3)
    from_left_top, from_right_low = shift(right_top + far_top, 1), shift(left_low + far_low, 3)
    return mine + jnp.concatenate([from_left_top + from_right_top, from_left_low + from_right_low], 0)


def cycle(residual, psf, positions):
    nrows = lax.axis_size(ROWS)
    slab, ncols = residual.shape[1:]
    z = lax.axis_index("rows_0")
    outer = (z == 0) | (z == 3)
    pos = positions.T
    own = psf[0]
    to_outer, to_inner = permute(own, OUTER), permute(own, INNER)
    own1, own3, own2 = (permute(own, turn(by, lambda z, y: 4 * z + y)) for by in (1, 3, 2))
    far = permute(own, ACROSS)
    parts = table(pos, own, residual[0])
    near = jnp.where(outer, to_outer, to_inner)
    near1, near3 = (permute(near, turn(by, near_held)) for by in (1, 3))
    parts, near = lax.optimization_barrier((parts, near))
    parts = lax.all_to_all(parts, CHAN_ROWS, 0, 0, tiled=True)
    far1, far2, far3 = (permute(far, turn(by, halfway_held)) for by in (1, 2, 3))
    near2_outer, near2_inner = permute(own2, OUTER), permute(own2, INNER)
    amps = solve(parts)
    early = (own, own1, own2, own3, near, near1, near3)
    mine, yours = part(EARLY, (0, 1), False, pos, amps, early, (residual[0],))
    rest = (near2_outer, near2_inner, far, far1, far2, far3)
    (yours,) = part(LATE, (1,), True, pos, amps, rest, (yours,))
    other = lax.ppermute(yours, "rows_2", [(0, 1), (1, 0)])
    (mine,) = part(LATE, (0,), True, pos, amps, rest, (mine,))
    image, *pieces = join(mine, other)
    summed = channel_sum(pieces)
    square = jnp.broadcast_to(jnp.sum(summed * summed), (DEVICES, 1, LANES))
    total = jnp.sum(lax.all_to_all(square, CHAN_ROWS, 0, 0, tiled=True)[:, 0, 0])
    count = slab * nrows * ncols
    normalized = summed * lax.rsqrt(total / count + 1e-06)
    return (image[None], normalized)


def solution(mesh):
    finer = Mesh(
        mesh.devices.reshape(mesh.shape["chan"], 4, 4, 2), ("chan", "rows_0", "rows_1", "rows_2")
    )
    return jax.shard_map(
        cycle,
        mesh=finer,
        in_specs=(P("chan", ROWS, None), P("chan", ROWS, None), P()),
        out_specs=(P("chan", ROWS, None), P(ROWS, "chan")),
        check_vma=False,
    )
```

```python
import functools

import jax
import jax.numpy as jnp
from jax import lax
from jax.experimental import pallas as pl
from jax.experimental.pallas import tpu as pltpu
from jax.sharding import Mesh
from jax.sharding import PartitionSpec as P


STEPS = 32
ROWS = ("rows_0", "rows_1", "rows_2")
CHAN_ROWS = ("chan", "rows_0", "rows_1", "rows_2")
LANES = 128
SUBLANES = 8
DEVICES = 128
NCHAN = 4
SLAB = 32
SHARD = 64
PATCH = 2048
HALF = PATCH // 2
NCOL = 16384
TALL = SLAB + SUBLANES
FOLD = LANES // STEPS
QUARTER = NCOL // NCHAN
SLOTS = 10
EDGE = 32
PART_VMEM = 40 << 20
JOIN_VMEM = 12 << 20
EARLY = (("own", 0), ("own", 1), ("own", 2), ("own", 3), ("near", 0), ("near", 1), ("near", 3))
LATE = (("near_outer", 2), ("near_inner", 2), ("far", 0), ("far", 1), ("far", 2), ("far", 3))
PIECES = (
    (0, 0, 32),
    (1, 0, 16),
    (1, 16, 16),
    (2, 0, 16),
    (2, 16, 16),
    (3, 0, 16),
    (3, 16, 16),
)


def place_of_rows():
    return lax.axis_index("rows_0") * 8 + lax.axis_index("rows_1") * 2 + lax.axis_index("rows_2")


def floor_to(x, size):
    return pl.multiple_of(x - (x & (size - 1)), size)


def table_kernel(pos_ref, psf_ref, res_ref, out_ref, tiles, wide, acc, sems):
    row_id = place_of_rows()
    first = row_id * SLAB
    lane = lax.broadcasted_iota(jnp.int32, (SUBLANES, LANES), 1)
    cell = lax.broadcasted_iota(jnp.int32, (SUBLANES, LANES), 0) * LANES + lane

    def tile_copy(k):
        local = (pos_ref[0, k] - first) & (SLAB - 1)
        src = res_ref.at[pl.ds(floor_to(local, SUBLANES), SUBLANES), pl.ds(floor_to(pos_ref[1, k], LANES), LANES)]
        return pltpu.make_async_copy(src, tiles.at[k], sems.at[k])

    def placed(tile, row, col, target, foreign):
        turned = pltpu.roll(tile, (target - col) & (LANES - 1), 1)
        code = (row & (SUBLANES - 1)) * LANES + target
        return cell == jnp.where(foreign == 0, code, -1), turned

    for k in range(STEPS):
        tile_copy(k).start()
    sums = [jnp.zeros((SUBLANES, LANES), jnp.float32) for _ in range(STEPS // FOLD)]
    for k in range(STEPS):
        base_row = pos_ref[0, k] + (HALF - row_id * SHARD)
        base_col = pos_ref[1, k] + HALF
        for l in range(k):
            row = base_row - pos_ref[0, l]
            col = base_col - pos_ref[1, l]
            foreign = (row >> 6) | (col >> 11)
            rows = pl.ds(pl.multiple_of(row & (SHARD - SUBLANES), SUBLANES), SUBLANES)
            cols = pl.ds(pl.multiple_of(col & (PATCH - LANES), LANES), LANES)
            here, turned = placed(psf_ref[rows, cols], row, col, STEPS * (k % FOLD) + l, foreign)
            sums[k // FOLD] = jnp.where(here, turned, sums[k // FOLD])
        if k % FOLD == FOLD - 1:
            wide[k // FOLD] = sums[k // FOLD]
    for k in range(STEPS):
        tile_copy(k).wait()
        local = pos_ref[0, k] - first
        here, turned = placed(tiles[k], local, pos_ref[1, k], STEPS * (k % FOLD) + k, local >> 5)
        wide[k // FOLD] = jnp.where(here, turned, wide[k // FOLD])
    for g in range(STEPS // FOLD):
        acc[g : g + 1, :] = jnp.sum(wide[g], axis=0, keepdims=True)
    out_ref[...] = jnp.broadcast_to(acc[...][None], (DEVICES, SUBLANES, LANES))


def table(pos, psf, residual):
    return pl.pallas_call(
        table_kernel,
        out_shape=jax.ShapeDtypeStruct((DEVICES, SUBLANES, LANES), jnp.float32),
        in_specs=[
            pl.BlockSpec(memory_space=pltpu.SMEM),
            pl.BlockSpec(memory_space=pltpu.VMEM),
            pl.BlockSpec(memory_space=pl.ANY),
        ],
        out_specs=pl.BlockSpec(memory_space=pltpu.VMEM),
        scratch_shapes=[
            pltpu.VMEM((STEPS, SUBLANES, LANES), jnp.float32),
            pltpu.VMEM((SUBLANES, SUBLANES, LANES), jnp.float32),
            pltpu.VMEM((SUBLANES, LANES), jnp.float32),
            pltpu.SemaphoreType.DMA((STEPS,)),
        ],
        name="table",
    )(pos, psf, residual)


def solve(parts_ref, amps_ref, rows):
    chan_id = lax.axis_index("chan")
    per_chan = DEVICES // NCHAN
    for c in range(NCHAN):
        sums = [parts_ref[c * per_chan + d] for d in range(per_chan)]
        while len(sums) > 1:
            sums = [a + b for a, b in zip(sums[::2], sums[1::2])]
        for g in range(SUBLANES):
            rows[g, c : c + 1, :] = sums[0][g : g + 1, :]
            rows[g, NCHAN + c : NCHAN + c + 1, :] = jnp.zeros((1, LANES), jnp.float32)
    lane = lax.broadcasted_iota(jnp.int32, (SUBLANES, LANES), 1)
    sub = lax.broadcasted_iota(jnp.int32, (SUBLANES, LANES), 0)
    at = lane % STEPS
    group = lane // STEPS
    own = sub == chan_id
    amps = jnp.zeros((SUBLANES, LANES), jnp.float32)
    for k in range(STEPS):
        weights = jnp.where(at == k, -1.0, amps)
        products = jnp.where(group == k % FOLD, rows[k // FOLD] * weights, 0.0)
        value = -jnp.sum(products, axis=1, keepdims=True)
        total = jnp.sum(value, axis=0, keepdims=True)
        amp = jnp.broadcast_to(0.25 * (value + total / NCHAN), (SUBLANES, LANES))
        amps = jnp.where((at == k) & (sub < NCHAN), amp, amps)
        mine = jnp.sum(jnp.where(own, amp, 0.0), axis=0, keepdims=True)
        amps_ref[k] = jnp.broadcast_to(mine, (SUBLANES, LANES))


NEAR = (1, 2, 1, 2)
HALFWAY = (2, 0, 3, 1)


def place(z, y, c):
    return z * 8 + y * 2 + c


def needs(z, y, c, j):
    return 4 * z + y <= 2 * j + c <= 4 * z + y + 16


def near_held(z, y):
    return 4 * NEAR[z] + y


def halfway_held(z, y):
    return 4 * HALFWAY[z] + y if (y < 2) == (z % 2 == 0) else None


def turn(by, held):
    chips = [(z, y) for z in range(4) for y in range(4) if held(z, y) is not None]
    return [
        (place(z, y, c), place(z, (y + by) % 4, c))
        for z, y in chips
        for c in range(2)
        if needs(z, (y + by) % 4, c, held(z, y))
    ]


def climb(moves):
    return [(place(a, y, c), place(b, y, c)) for a, b in moves for y in range(4) for c in range(2)]


OUTER = climb([(1, 0), (2, 3)])
INNER = climb([(2, 1), (1, 2)])
ACROSS = [
    (place(HALFWAY[z], y, c), place(z, y, c))
    for z in range(4)
    for y in range(4)
    for c in range(2)
    if halfway_held(z, y) is not None
]


ACROSS_TWO = [
    (place(HALFWAY[z], (y + 2) % 4, c), place(z, (y + 2) % 4, c))
    for z in range(4)
    for y in range(4)
    for c in range(2)
    if halfway_held(z, y) is not None and needs(z, (y + 2) % 4, c, halfway_held(z, y))
]


def permute(x, pairs):
    return lax.ppermute(x, ROWS, pairs)


def part_kernel(names, halves, late, from_residual, pos_ref, amps_ref, *rest):
    if from_residual:
        parts_ref, (rest, parts, amps_rows, parts_sems) = amps_ref, (rest[:-3], *rest[-3:])
        amps_ref = rest[len(names) + 1]
        rest = (*rest[: len(names) + 1], *rest[len(names) + 2 :])
    count = len(names)
    block_refs, rest = rest[:count], rest[count:]
    base_refs, rest = rest[: 1 if from_residual else len(halves)], rest[1 if from_residual else len(halves) :]
    out_refs, rest = rest[: len(halves)], rest[len(halves) :]
    images, (patch, sems, edge_sems) = rest[: len(halves)], rest[len(halves) :]
    z, y, c = (lax.axis_index(name) for name in ROWS)
    inner = (z == 1) | (z == 2)
    odd = z & 1
    near_slot = jnp.where(z == 0, 4, jnp.where(z == 1, 6, jnp.where(z == 2, 0, 2)))
    far_slot = jnp.where(odd == 0, 8, -2)
    lane = lax.broadcasted_iota(jnp.int32, (SUBLANES, LANES), 1)
    sub = lax.broadcasted_iota(jnp.int32, (SUBLANES, LANES), 0)

    def each_block(act):
        for i, (kind, by) in enumerate(names):
            source = (y - by) & 3
            if kind == "own":
                slot, held = 2 * z + source, None
            elif kind == "far":
                slot, held = far_slot + source, (source >> 1) == odd
            else:
                slot = near_slot + source
                held = None if kind == "near" else inner == (kind == "near_inner")
            slot = jnp.clip(slot, 0, SLOTS - 1)
            rows = pl.ds(pl.multiple_of(EDGE + slot * SHARD, SUBLANES), SHARD)
            copy = pltpu.make_async_copy(block_refs[i], patch.at[rows, :], sems.at[i])
            if held is None:
                act(copy)
            else:
                pl.when(held)(functools.partial(act, copy))

    if from_residual:
        parts_load = pltpu.make_async_copy(parts_ref, parts, parts_sems.at[0])
        parts_load.start()
    each_block(lambda copy: copy.start())
    loads = []
    for n, image in enumerate(images):
        if from_residual and halves[n] == 1:
            image[...] = jnp.zeros(image.shape, jnp.float32)
        else:
            base = base_refs[0 if from_residual else n]
            loads.append(pltpu.make_async_copy(base, image.at[:, pl.ds(0, NCOL)], edge_sems.at[n]))
            loads[-1].start()
    if from_residual:
        parts_load.wait()
        solve(parts, amps_ref, amps_rows)
    each_block(lambda copy: copy.wait())
    for load in loads:
        load.wait()

    def peak(image, first, k):
        start = first - pos_ref[0, k] + HALF
        other = ((start >> 6) ^ c) & 1
        skew = (start & (SHARD - 1)) - other * SHARD
        slot = (((start >> 6) + other) >> 1) - 2 * z
        is_late = ((slot >> 1) == jnp.where(odd == 0, 4, 0)) | (slot == near_slot + ((y + 2) & 3))

        @pl.when((skew > -SLAB) & (is_late == late))
        def _():
            row = EDGE + slot * SHARD + skew
            off = row & (SUBLANES - 1)
            row = row - off
            left = pos_ref[1, k] - HALF
            shift = left & (LANES - 1)
            base = left - shift
            amp = amps_ref[k]
            carried = lane < shift
            upper = sub < SUBLANES - off
            groups = TALL // SUBLANES
            places = [sub + (g * SUBLANES + skew) for g in range(SLAB // SUBLANES)]
            within = [(at >= 0) & (at < SHARD) for at in places]
            back = (SUBLANES - off) & (SUBLANES - 1)
            before = [jnp.zeros((SUBLANES, LANES), jnp.float32)] * (groups - 1)
            for t in range(PATCH // LANES + 1):
                if t < PATCH // LANES:
                    raised = []
                    for g in range(groups):
                        rows = pl.ds(pl.multiple_of(row + g * SUBLANES, SUBLANES), SUBLANES)
                        raised.append(pltpu.roll(patch[rows, pl.ds(t * LANES, LANES)], back, 0))
                    joined = [jnp.where(upper, raised[g], raised[g + 1]) for g in range(groups - 1)]
                    turned = [pltpu.roll(x, shift, 1) for x in joined]
                else:
                    turned = [jnp.zeros((SUBLANES, LANES), jnp.float32)] * (groups - 1)
                cols = pl.ds(pl.multiple_of(base + t * LANES, LANES), LANES)
                for g in range(groups - 1):
                    rows = pl.ds(g * SUBLANES, SUBLANES)
                    value = jnp.where(within[g], jnp.where(carried, before[g], turned[g]), 0.0)
                    image[rows, cols] = image[rows, cols] - amp * value
                before = turned

    stores = []
    for n, image in enumerate(images):
        half = c if halves[n] == 0 else 1 - c
        first = (4 * z + y) * SHARD + half * SLAB
        lax.fori_loop(0, STEPS, lambda k, _, image=image, first=first: (peak(image, first, k), 0)[1], 0)
        stores.append(pltpu.make_async_copy(image.at[:, pl.ds(0, NCOL)], out_refs[n], edge_sems.at[n]))
        stores[-1].start()
    for store in stores:
        store.wait()


def part(names, halves, late, pos, amps, blocks, bases):
    anywhere = pl.BlockSpec(memory_space=pl.ANY)
    vmem = pl.BlockSpec(memory_space=pltpu.VMEM)
    images = [jax.ShapeDtypeStruct((SLAB, NCOL), jnp.float32)] * len(halves)
    solved = [] if late else [jax.ShapeDtypeStruct((STEPS, SUBLANES, LANES), jnp.float32)]
    solving = [
        pltpu.VMEM((DEVICES, SUBLANES, LANES), jnp.float32),
        pltpu.VMEM((SUBLANES, SUBLANES, LANES), jnp.float32),
        pltpu.SemaphoreType.DMA((1,)),
    ]
    return pl.pallas_call(
        functools.partial(part_kernel, names, halves, late, not late),
        out_shape=solved + images,
        in_specs=[pl.BlockSpec(memory_space=pltpu.SMEM), vmem if late else anywhere]
        + [anywhere] * (len(blocks) + len(bases)),
        out_specs=[vmem] * len(solved) + [anywhere] * len(halves),
        scratch_shapes=[pltpu.VMEM((SLAB, NCOL + LANES), jnp.float32)] * len(halves)
        + [
            pltpu.VMEM((2 * EDGE + SLOTS * SHARD, PATCH), jnp.float32),
            pltpu.SemaphoreType.DMA((len(names),)),
            pltpu.SemaphoreType.DMA((len(halves),)),
        ]
        + ([] if late else solving),
        compiler_params=pltpu.CompilerParams(vmem_limit_bytes=PART_VMEM),
    )(pos, amps, *blocks, *bases)


def join_kernel(mine_ref, other_ref, out_ref, *rest):
    piece_refs, (mine, other, sems, piece_sems) = rest[: len(PIECES)], rest[len(PIECES) :]
    chan_id = lax.axis_index("chan")

    def cols(ahead):
        return pl.ds(pl.multiple_of(((chan_id + ahead) & (NCHAN - 1)) * QUARTER, QUARTER), QUARTER)

    def load(ahead, n):
        src, dst = ((mine_ref, mine), (other_ref, other))[n]
        return pltpu.make_async_copy(src.at[:, cols(ahead)], dst.at[ahead], sems.at[n, ahead])

    order = (2, 1, 3, 0)
    for ahead in order:
        load(ahead, 0).start()
        load(ahead, 1).start()
    stores = []
    for ahead in order:
        load(ahead, 0).wait()
        load(ahead, 1).wait()
        mine[ahead] = mine[ahead] + other[ahead]
        stores.append(pltpu.make_async_copy(mine.at[ahead], out_ref.at[:, cols(ahead)], sems.at[2, ahead]))
        stores[-1].start()
        for i, (where, top, tall) in enumerate(PIECES):
            if where == ahead:
                src = mine.at[ahead, pl.ds(top, tall), :]
                stores.append(pltpu.make_async_copy(src, piece_refs[i], piece_sems.at[i]))
                stores[-1].start()
    for store in stores:
        store.wait()


def join(mine, other):
    anywhere = pl.BlockSpec(memory_space=pl.ANY)
    return pl.pallas_call(
        join_kernel,
        out_shape=[
            jax.ShapeDtypeStruct((SLAB, NCOL), jnp.float32),
            *(jax.ShapeDtypeStruct((tall, QUARTER), jnp.float32) for _, _, tall in PIECES),
        ],
        in_specs=[anywhere] * 2,
        out_specs=[anywhere] * (len(PIECES) + 1),
        scratch_shapes=[
            pltpu.VMEM((NCHAN, SLAB, QUARTER), jnp.float32),
            pltpu.VMEM((NCHAN, SLAB, QUARTER), jnp.float32),
            pltpu.SemaphoreType.DMA((3, NCHAN)),
            pltpu.SemaphoreType.DMA((len(PIECES),)),
        ],
        compiler_params=pltpu.CompilerParams(vmem_limit_bytes=JOIN_VMEM),
        name="join",
    )(mine, other)


def channel_sum(pieces):
    mine, right_top, right_low, far_top, far_low, left_top, left_low = pieces

    def shift(x, by):
        return lax.ppermute(x, "chan", [(i, (i + by) % NCHAN) for i in range(NCHAN)])

    far_top, far_low = shift(far_top, 1), shift(far_low, 3)
    from_left_low, from_right_top = shift(right_low, 1), shift(left_top, 3)
    from_left_top, from_right_low = shift(right_top + far_top, 1), shift(left_low + far_low, 3)
    return mine + jnp.concatenate([from_left_top + from_right_top, from_left_low + from_right_low], 0)


def cycle(residual, psf, positions):
    nrows = lax.axis_size(ROWS)
    slab, ncols = residual.shape[1:]
    z = lax.axis_index("rows_0")
    outer = (z == 0) | (z == 3)
    pos = positions.T
    own = psf[0]
    to_outer, to_inner = permute(own, OUTER), permute(own, INNER)
    own1, own3, own2 = (permute(own, turn(by, lambda z, y: 4 * z + y)) for by in (1, 3, 2))
    far = permute(own, ACROSS)
    parts = table(pos, own, residual[0])
    near = jnp.where(outer, to_outer, to_inner)
    near1, near3 = (permute(near, turn(by, near_held)) for by in (1, 3))
    parts = lax.all_to_all(parts, CHAN_ROWS, 0, 0, tiled=True)
    far1, far3 = (permute(far, turn(by, halfway_held)) for by in (1, 3))
    far2 = permute(own2, ACROSS_TWO)
    near2_outer, near2_inner = permute(own2, OUTER), permute(own2, INNER)
    early = (own, own1, own2, own3, near, near1, near3)
    amps, mine, yours = part(EARLY, (0, 1), False, pos, parts, early, (residual[0],))
    rest = (near2_outer, near2_inner, far, far1, far2, far3)
    (yours,) = part(LATE, (1,), True, pos, amps, rest, (yours,))
    other = lax.ppermute(yours, "rows_2", [(0, 1), (1, 0)])
    (mine,) = part(LATE, (0,), True, pos, amps, rest, (mine,))
    image, *pieces = join(mine, other)
    summed = channel_sum(pieces)
    square = jnp.broadcast_to(jnp.sum(summed * summed), (DEVICES, 1, LANES))
    total = jnp.sum(lax.all_to_all(square, CHAN_ROWS, 0, 0, tiled=True)[:, 0, 0])
    count = slab * nrows * ncols
    normalized = summed * lax.rsqrt(total / count + 1e-06)
    return (image[None], normalized)


def solution(mesh):
    finer = Mesh(
        mesh.devices.reshape(mesh.shape["chan"], 4, 4, 2), ("chan", "rows_0", "rows_1", "rows_2")
    )
    return jax.shard_map(
        cycle,
        mesh=finer,
        in_specs=(P("chan", ROWS, None), P("chan", ROWS, None), P()),
        out_specs=(P("chan", ROWS, None), P(ROWS, "chan")),
        check_vma=False,
    )
```

```python
import functools

import jax
import jax.numpy as jnp
from jax import lax
from jax.experimental import pallas as pl
from jax.experimental.pallas import tpu as pltpu
from jax.sharding import Mesh
from jax.sharding import PartitionSpec as P


STEPS = 32
ROWS = ("rows_0", "rows_1", "rows_2")
CHAN_ROWS = ("chan", "rows_0", "rows_1", "rows_2")
LANES = 128
SUBLANES = 8
DEVICES = 128
NCHAN = 4
SLAB = 32
SHARD = 64
PATCH = 2048
HALF = PATCH // 2
NCOL = 16384
TALL = SLAB + SUBLANES
FOLD = LANES // STEPS
QUARTER = NCOL // NCHAN
SLOTS = 10
EDGE = 32
PART_VMEM = 40 << 20
JOIN_VMEM = 12 << 20
EARLY = (("own", 0), ("own", 1), ("own", 2), ("own", 3), ("near", 0), ("near", 1), ("near", 3))
LATE = (("near_outer", 2), ("near_inner", 2), ("far", 0), ("far", 1), ("far", 2), ("far", 3))
PIECES = (
    (0, 0, 32),
    (1, 0, 16),
    (1, 16, 16),
    (2, 0, 16),
    (2, 16, 16),
    (3, 0, 16),
    (3, 16, 16),
)


def place_of_rows():
    return lax.axis_index("rows_0") * 8 + lax.axis_index("rows_1") * 2 + lax.axis_index("rows_2")


def floor_to(x, size):
    return pl.multiple_of(x - (x & (size - 1)), size)


def table_kernel(pos_ref, psf_ref, res_ref, out_ref, tiles, acc, packed, sems):
    row_id = place_of_rows()
    first = row_id * SLAB
    lane = lax.broadcasted_iota(jnp.int32, (SUBLANES, LANES), 1)
    cell = lax.broadcasted_iota(jnp.int32, (SUBLANES, LANES), 0) * LANES + lane

    def tile_copy(k):
        local = (pos_ref[0, k] - first) & (SLAB - 1)
        src = res_ref.at[pl.ds(floor_to(local, SUBLANES), SUBLANES), pl.ds(floor_to(pos_ref[1, k], LANES), LANES)]
        return pltpu.make_async_copy(src, tiles.at[k], sems.at[k])

    def placed(tile, row, col, target, foreign):
        turned = pltpu.roll(tile, (target - col) & (LANES - 1), 1)
        code = (row & (SUBLANES - 1)) * LANES + target
        return cell == jnp.where(foreign == 0, code, -1), turned

    for k in range(STEPS):
        tile_copy(k).start()
    sums = [jnp.zeros((SUBLANES, LANES), jnp.float32) for _ in range(STEPS // FOLD)]
    for k in range(STEPS):
        packed[k] = (pos_ref[0, k] << 16) + pos_ref[1, k]
    corner = ((HALF - row_id * SHARD) << 16) + HALF
    for k in range(STEPS):
        base = packed[k] + corner
        for l in range(k):
            place_of = base - packed[l]
            foreign = place_of & -0x3F0800
            rows = pl.ds(pl.multiple_of((place_of >> 16) & (SHARD - SUBLANES), SUBLANES), SUBLANES)
            cols = pl.ds(pl.multiple_of(place_of & (PATCH - LANES), LANES), LANES)
            target = STEPS * (k % FOLD) + l
            turned = pltpu.roll(psf_ref[rows, cols], (target - place_of) & (LANES - 1), 1)
            code = ((place_of >> 9) & ((SUBLANES - 1) * LANES)) + target
            here = cell == jnp.where(foreign == 0, code, -1)
            sums[k // FOLD] = jnp.where(here, turned, sums[k // FOLD])
    for k in range(STEPS):
        tile_copy(k).wait()
    for k in range(STEPS):
        local = pos_ref[0, k] - first
        here, turned = placed(tiles[k], local, pos_ref[1, k], STEPS * (k % FOLD) + k, local >> 5)
        sums[k // FOLD] = jnp.where(here, turned, sums[k // FOLD])
    for g in range(STEPS // FOLD):
        acc[g : g + 1, :] = jnp.sum(sums[g], axis=0, keepdims=True)
    out_ref[...] = jnp.broadcast_to(acc[...][None], (DEVICES, SUBLANES, LANES))


def table(pos, psf, residual):
    return pl.pallas_call(
        table_kernel,
        out_shape=jax.ShapeDtypeStruct((DEVICES, SUBLANES, LANES), jnp.float32),
        in_specs=[
            pl.BlockSpec(memory_space=pltpu.SMEM),
            pl.BlockSpec(memory_space=pltpu.VMEM),
            pl.BlockSpec(memory_space=pl.ANY),
        ],
        out_specs=pl.BlockSpec(memory_space=pltpu.VMEM),
        scratch_shapes=[
            pltpu.VMEM((STEPS, SUBLANES, LANES), jnp.float32),
            pltpu.VMEM((SUBLANES, LANES), jnp.float32),
            pltpu.SMEM((STEPS,), jnp.int32),
            pltpu.SemaphoreType.DMA((STEPS,)),
        ],
        name="table",
    )(pos, psf, residual)


def solve(parts_ref, amps_ref, rows):
    chan_id = lax.axis_index("chan")
    per_chan = DEVICES // NCHAN
    for c in range(NCHAN):
        sums = [parts_ref[c * per_chan + d] for d in range(per_chan)]
        while len(sums) > 1:
            sums = [a + b for a, b in zip(sums[::2], sums[1::2])]
        for g in range(SUBLANES):
            rows[g, c : c + 1, :] = sums[0][g : g + 1, :]
            rows[g, NCHAN + c : NCHAN + c + 1, :] = jnp.zeros((1, LANES), jnp.float32)
    sub = lax.broadcasted_iota(jnp.int32, (SUBLANES, LANES), 0)
    own = sub == chan_id
    amps = []
    for k in range(STEPS):
        line = rows[k // FOLD]
        at = STEPS * (k % FOLD)
        spread = [jnp.broadcast_to(line[:, at + l : at + l + 1], (SUBLANES, LANES)) for l in range(k + 1)]
        value = spread[k]
        for l in range(k):
            value = value - spread[l] * amps[l]
        total = jnp.sum(value, axis=0, keepdims=True)
        amp = 0.25 * (value + total / NCHAN)
        amps.append(jnp.where(sub < NCHAN, amp, 0.0))
        mine = jnp.sum(jnp.where(own, amp, 0.0), axis=0, keepdims=True)
        amps_ref[k] = jnp.broadcast_to(mine, (SUBLANES, LANES))


NEAR = (1, 2, 1, 2)
HALFWAY = (2, 0, 3, 1)


def place(z, y, c):
    return z * 8 + y * 2 + c


def needs(z, y, c, j):
    return 4 * z + y <= 2 * j + c <= 4 * z + y + 16


def near_held(z, y):
    return 4 * NEAR[z] + y


def halfway_held(z, y):
    return 4 * HALFWAY[z] + y if (y < 2) == (z % 2 == 0) else None


def turn(by, held):
    chips = [(z, y) for z in range(4) for y in range(4) if held(z, y) is not None]
    return [
        (place(z, y, c), place(z, (y + by) % 4, c))
        for z, y in chips
        for c in range(2)
        if needs(z, (y + by) % 4, c, held(z, y))
    ]


def climb(moves):
    return [(place(a, y, c), place(b, y, c)) for a, b in moves for y in range(4) for c in range(2)]


OUTER = climb([(1, 0), (2, 3)])
INNER = climb([(2, 1), (1, 2)])
ACROSS = [
    (place(HALFWAY[z], y, c), place(z, y, c))
    for z in range(4)
    for y in range(4)
    for c in range(2)
    if halfway_held(z, y) is not None
]


ACROSS_TWO = [
    (place(HALFWAY[z], (y + 2) % 4, c), place(z, (y + 2) % 4, c))
    for z in range(4)
    for y in range(4)
    for c in range(2)
    if halfway_held(z, y) is not None and needs(z, (y + 2) % 4, c, halfway_held(z, y))
]


def permute(x, pairs):
    return lax.ppermute(x, ROWS, pairs)


def part_kernel(names, halves, late, from_residual, pos_ref, amps_ref, *rest):
    if from_residual:
        parts_ref, (rest, parts, amps_rows, parts_sems) = amps_ref, (rest[:-3], *rest[-3:])
        amps_ref = rest[len(names) + 1]
        rest = (*rest[: len(names) + 1], *rest[len(names) + 2 :])
    count = len(names)
    block_refs, rest = rest[:count], rest[count:]
    base_refs, rest = rest[: 1 if from_residual else len(halves)], rest[1 if from_residual else len(halves) :]
    out_refs, rest = rest[: len(halves)], rest[len(halves) :]
    images, (patch, sems, edge_sems) = rest[: len(halves)], rest[len(halves) :]
    z, y, c = (lax.axis_index(name) for name in ROWS)
    inner = (z == 1) | (z == 2)
    odd = z & 1
    near_slot = jnp.where(z == 0, 4, jnp.where(z == 1, 6, jnp.where(z == 2, 0, 2)))
    far_slot = jnp.where(odd == 0, 8, -2)
    lane = lax.broadcasted_iota(jnp.int32, (SUBLANES, LANES), 1)
    sub = lax.broadcasted_iota(jnp.int32, (SUBLANES, LANES), 0)

    def each_block(act):
        for i, (kind, by) in enumerate(names):
            source = (y - by) & 3
            if kind == "own":
                slot, held = 2 * z + source, None
            elif kind == "far":
                slot, held = far_slot + source, (source >> 1) == odd
            else:
                slot = near_slot + source
                held = None if kind == "near" else inner == (kind == "near_inner")
            slot = jnp.clip(slot, 0, SLOTS - 1)
            rows = pl.ds(pl.multiple_of(EDGE + slot * SHARD, SUBLANES), SHARD)
            copy = pltpu.make_async_copy(block_refs[i], patch.at[rows, :], sems.at[i])
            if held is None:
                act(copy)
            else:
                pl.when(held)(functools.partial(act, copy))

    if from_residual:
        parts_load = pltpu.make_async_copy(parts_ref, parts, parts_sems.at[0])
        parts_load.start()
    each_block(lambda copy: copy.start())
    loads = []
    for n, image in enumerate(images):
        if from_residual and halves[n] == 1:
            image[...] = jnp.zeros(image.shape, jnp.float32)
        else:
            base = base_refs[0 if from_residual else n]
            loads.append(pltpu.make_async_copy(base, image.at[:, pl.ds(0, NCOL)], edge_sems.at[n]))
            loads[-1].start()
    if from_residual:
        parts_load.wait()
        solve(parts, amps_ref, amps_rows)
    each_block(lambda copy: copy.wait())
    for load in loads:
        load.wait()

    def peak(image, first, k):
        start = first - pos_ref[0, k] + HALF
        other = ((start >> 6) ^ c) & 1
        skew = (start & (SHARD - 1)) - other * SHARD
        slot = (((start >> 6) + other) >> 1) - 2 * z
        is_late = ((slot >> 1) == jnp.where(odd == 0, 4, 0)) | (slot == near_slot + ((y + 2) & 3))

        @pl.when((skew > -SLAB) & (is_late == late))
        def _():
            row = EDGE + slot * SHARD + skew
            off = row & (SUBLANES - 1)
            row = row - off
            left = pos_ref[1, k] - HALF
            shift = left & (LANES - 1)
            base = left - shift
            amp = amps_ref[k]
            carried = lane < shift
            upper = sub < SUBLANES - off
            groups = TALL // SUBLANES
            places = [sub + (g * SUBLANES + skew) for g in range(SLAB // SUBLANES)]
            within = [(at >= 0) & (at < SHARD) for at in places]
            back = (SUBLANES - off) & (SUBLANES - 1)
            before = [jnp.zeros((SUBLANES, LANES), jnp.float32)] * (groups - 1)
            for t in range(PATCH // LANES + 1):
                if t < PATCH // LANES:
                    raised = []
                    for g in range(groups):
                        rows = pl.ds(pl.multiple_of(row + g * SUBLANES, SUBLANES), SUBLANES)
                        raised.append(pltpu.roll(patch[rows, pl.ds(t * LANES, LANES)], back, 0))
                    joined = [jnp.where(upper, raised[g], raised[g + 1]) for g in range(groups - 1)]
                    turned = [pltpu.roll(x, shift, 1) for x in joined]
                else:
                    turned = [jnp.zeros((SUBLANES, LANES), jnp.float32)] * (groups - 1)
                cols = pl.ds(pl.multiple_of(base + t * LANES, LANES), LANES)
                for g in range(groups - 1):
                    rows = pl.ds(g * SUBLANES, SUBLANES)
                    value = jnp.where(within[g], jnp.where(carried, before[g], turned[g]), 0.0)
                    image[rows, cols] = image[rows, cols] - amp * value
                before = turned

    stores = []
    for n, image in enumerate(images):
        half = c if halves[n] == 0 else 1 - c
        first = (4 * z + y) * SHARD + half * SLAB
        lax.fori_loop(0, STEPS, lambda k, _, image=image, first=first: (peak(image, first, k), 0)[1], 0)
        stores.append(pltpu.make_async_copy(image.at[:, pl.ds(0, NCOL)], out_refs[n], edge_sems.at[n]))
        stores[-1].start()
    for store in stores:
        store.wait()


def part(names, halves, late, pos, amps, blocks, bases):
    anywhere = pl.BlockSpec(memory_space=pl.ANY)
    vmem = pl.BlockSpec(memory_space=pltpu.VMEM)
    images = [jax.ShapeDtypeStruct((SLAB, NCOL), jnp.float32)] * len(halves)
    solved = [] if late else [jax.ShapeDtypeStruct((STEPS, SUBLANES, LANES), jnp.float32)]
    solving = [
        pltpu.VMEM((DEVICES, SUBLANES, LANES), jnp.float32),
        pltpu.VMEM((SUBLANES, SUBLANES, LANES), jnp.float32),
        pltpu.SemaphoreType.DMA((1,)),
    ]
    return pl.pallas_call(
        functools.partial(part_kernel, names, halves, late, not late),
        out_shape=solved + images,
        in_specs=[pl.BlockSpec(memory_space=pltpu.SMEM), vmem if late else anywhere]
        + [anywhere] * (len(blocks) + len(bases)),
        out_specs=[vmem] * len(solved) + [anywhere] * len(halves),
        scratch_shapes=[pltpu.VMEM((SLAB, NCOL + LANES), jnp.float32)] * len(halves)
        + [
            pltpu.VMEM((2 * EDGE + SLOTS * SHARD, PATCH), jnp.float32),
            pltpu.SemaphoreType.DMA((len(names),)),
            pltpu.SemaphoreType.DMA((len(halves),)),
        ]
        + ([] if late else solving),
        compiler_params=pltpu.CompilerParams(vmem_limit_bytes=PART_VMEM),
    )(pos, amps, *blocks, *bases)


def join_kernel(mine_ref, other_ref, out_ref, *rest):
    piece_refs, (mine, other, sems, piece_sems) = rest[: len(PIECES)], rest[len(PIECES) :]
    chan_id = lax.axis_index("chan")

    def cols(ahead):
        return pl.ds(pl.multiple_of(((chan_id + ahead) & (NCHAN - 1)) * QUARTER, QUARTER), QUARTER)

    def load(ahead, n):
        src, dst = ((mine_ref, mine), (other_ref, other))[n]
        return pltpu.make_async_copy(src.at[:, cols(ahead)], dst.at[ahead], sems.at[n, ahead])

    order = (2, 1, 3, 0)
    for ahead in order:
        load(ahead, 0).start()
        load(ahead, 1).start()
    stores = []
    for ahead in order:
        load(ahead, 0).wait()
        load(ahead, 1).wait()
        mine[ahead] = mine[ahead] + other[ahead]
        stores.append(pltpu.make_async_copy(mine.at[ahead], out_ref.at[:, cols(ahead)], sems.at[2, ahead]))
        stores[-1].start()
        for i, (where, top, tall) in enumerate(PIECES):
            if where == ahead:
                src = mine.at[ahead, pl.ds(top, tall), :]
                stores.append(pltpu.make_async_copy(src, piece_refs[i], piece_sems.at[i]))
                stores[-1].start()
    for store in stores:
        store.wait()


def join(mine, other):
    anywhere = pl.BlockSpec(memory_space=pl.ANY)
    return pl.pallas_call(
        join_kernel,
        out_shape=[
            jax.ShapeDtypeStruct((SLAB, NCOL), jnp.float32),
            *(jax.ShapeDtypeStruct((tall, QUARTER), jnp.float32) for _, _, tall in PIECES),
        ],
        in_specs=[anywhere] * 2,
        out_specs=[anywhere] * (len(PIECES) + 1),
        scratch_shapes=[
            pltpu.VMEM((NCHAN, SLAB, QUARTER), jnp.float32),
            pltpu.VMEM((NCHAN, SLAB, QUARTER), jnp.float32),
            pltpu.SemaphoreType.DMA((3, NCHAN)),
            pltpu.SemaphoreType.DMA((len(PIECES),)),
        ],
        compiler_params=pltpu.CompilerParams(vmem_limit_bytes=JOIN_VMEM),
        name="join",
    )(mine, other)


def channel_sum(pieces):
    mine, right_top, right_low, far_top, far_low, left_top, left_low = pieces

    def shift(x, by):
        return lax.ppermute(x, "chan", [(i, (i + by) % NCHAN) for i in range(NCHAN)])

    far_top, far_low = shift(far_top, 1), shift(far_low, 3)
    from_left_low, from_right_top = shift(right_low, 1), shift(left_top, 3)
    from_left_top, from_right_low = shift(right_top + far_top, 1), shift(left_low + far_low, 3)
    return mine + jnp.concatenate([from_left_top + from_right_top, from_left_low + from_right_low], 0)


def cycle(residual, psf, positions):
    nrows = lax.axis_size(ROWS)
    slab, ncols = residual.shape[1:]
    z = lax.axis_index("rows_0")
    outer = (z == 0) | (z == 3)
    pos = positions.T
    own = psf[0]
    to_outer, to_inner = permute(own, OUTER), permute(own, INNER)
    own1, own3, own2 = (permute(own, turn(by, lambda z, y: 4 * z + y)) for by in (1, 3, 2))
    far = permute(own, ACROSS)
    parts = table(pos, own, residual[0])
    near = jnp.where(outer, to_outer, to_inner)
    near1, near3 = (permute(near, turn(by, near_held)) for by in (1, 3))
    parts = lax.all_to_all(parts, CHAN_ROWS, 0, 0, tiled=True)
    far1, far3 = (permute(far, turn(by, halfway_held)) for by in (1, 3))
    far2 = permute(own2, ACROSS_TWO)
    near2_outer, near2_inner = permute(own2, OUTER), permute(own2, INNER)
    early = (own, own1, own2, own3, near, near1, near3)
    amps, mine, yours = part(EARLY, (0, 1), False, pos, parts, early, (residual[0],))
    rest = (near2_outer, near2_inner, far, far1, far2, far3)
    (yours,) = part(LATE, (1,), True, pos, amps, rest, (yours,))
    other = lax.ppermute(yours, "rows_2", [(0, 1), (1, 0)])
    (mine,) = part(LATE, (0,), True, pos, amps, rest, (mine,))
    image, *pieces = join(mine, other)
    summed = channel_sum(pieces)
    square = jnp.broadcast_to(jnp.sum(summed * summed), (DEVICES, 1, LANES))
    total = jnp.sum(lax.all_to_all(square, CHAN_ROWS, 0, 0, tiled=True)[:, 0, 0])
    count = slab * nrows * ncols
    normalized = summed * lax.rsqrt(total / count + 1e-06)
    return (image[None], normalized)


def solution(mesh):
    finer = Mesh(
        mesh.devices.reshape(mesh.shape["chan"], 4, 4, 2), ("chan", "rows_0", "rows_1", "rows_2")
    )
    return jax.shard_map(
        cycle,
        mesh=finer,
        in_specs=(P("chan", ROWS, None), P("chan", ROWS, None), P()),
        out_specs=(P("chan", ROWS, None), P(ROWS, "chan")),
        check_vma=False,
    )
```

```python
import functools

import jax
import jax.numpy as jnp
from jax import lax
from jax.experimental import pallas as pl
from jax.experimental.pallas import tpu as pltpu
from jax.sharding import Mesh
from jax.sharding import PartitionSpec as P


STEPS = 32
ROWS = ("rows_0", "rows_1", "rows_2")
CHAN_ROWS = ("chan", "rows_0", "rows_1", "rows_2")
LANES = 128
SUBLANES = 8
DEVICES = 128
NCHAN = 4
SLAB = 32
SHARD = 64
PATCH = 2048
HALF = PATCH // 2
NCOL = 16384
TALL = SLAB + SUBLANES
FOLD = LANES // STEPS
QUARTER = NCOL // NCHAN
SLOTS = 10
EDGE = 32
PART_VMEM = 13 << 20
JOIN_VMEM = 6 << 20
EARLY = (("own", 0), ("own", 1), ("own", 2), ("own", 3), ("near", 0), ("near", 1), ("near", 3))
LATE = (("near_outer", 2), ("near_inner", 2), ("far", 0), ("far", 1), ("far", 2), ("far", 3))
PIECES = (
    (0, 0, 32),
    (1, 0, 16),
    (1, 16, 16),
    (2, 0, 16),
    (2, 16, 16),
    (3, 0, 16),
    (3, 16, 16),
)


def place_of_rows():
    return lax.axis_index("rows_0") * 8 + lax.axis_index("rows_1") * 2 + lax.axis_index("rows_2")


def floor_to(x, size):
    return pl.multiple_of(x - (x & (size - 1)), size)


def table_kernel(pos_ref, psf_ref, res_ref, out_ref, tiles, acc, packed, sems):
    row_id = place_of_rows()
    first = row_id * SLAB
    lane = lax.broadcasted_iota(jnp.int32, (SUBLANES, LANES), 1)
    cell = lax.broadcasted_iota(jnp.int32, (SUBLANES, LANES), 0) * LANES + lane

    def tile_copy(k):
        local = (pos_ref[0, k] - first) & (SLAB - 1)
        src = res_ref.at[pl.ds(floor_to(local, SUBLANES), SUBLANES), pl.ds(floor_to(pos_ref[1, k], LANES), LANES)]
        return pltpu.make_async_copy(src, tiles.at[k], sems.at[k])

    def placed(tile, row, col, target, foreign):
        turned = pltpu.roll(tile, (target - col) & (LANES - 1), 1)
        code = (row & (SUBLANES - 1)) * LANES + target
        return cell == jnp.where(foreign == 0, code, -1), turned

    for k in range(STEPS):
        tile_copy(k).start()
    sums = [jnp.zeros((SUBLANES, LANES), jnp.float32) for _ in range(STEPS // FOLD)]
    for k in range(STEPS):
        packed[k] = (pos_ref[0, k] << 16) + pos_ref[1, k]
    corner = ((HALF - row_id * SHARD) << 16) + HALF
    for k in range(STEPS):
        base = packed[k] + corner
        for l in range(k):
            place_of = base - packed[l]
            foreign = place_of & -0x3F0800
            rows = pl.ds(pl.multiple_of((place_of >> 16) & (SHARD - SUBLANES), SUBLANES), SUBLANES)
            cols = pl.ds(pl.multiple_of(place_of & (PATCH - LANES), LANES), LANES)
            target = STEPS * (k % FOLD) + l
            turned = pltpu.roll(psf_ref[rows, cols], (target - place_of) & (LANES - 1), 1)
            code = ((place_of >> 9) & ((SUBLANES - 1) * LANES)) + target
            here = cell == jnp.where(foreign == 0, code, -1)
            sums[k // FOLD] = jnp.where(here, turned, sums[k // FOLD])
    for k in range(STEPS):
        tile_copy(k).wait()
    for k in range(STEPS):
        local = pos_ref[0, k] - first
        here, turned = placed(tiles[k], local, pos_ref[1, k], STEPS * (k % FOLD) + k, local >> 5)
        sums[k // FOLD] = jnp.where(here, turned, sums[k // FOLD])
    for g in range(STEPS // FOLD):
        acc[g : g + 1, :] = jnp.sum(sums[g], axis=0, keepdims=True)
    out_ref[...] = jnp.broadcast_to(acc[...][None], (DEVICES, SUBLANES, LANES))


def table(pos, psf, residual):
    return pl.pallas_call(
        table_kernel,
        out_shape=jax.ShapeDtypeStruct((DEVICES, SUBLANES, LANES), jnp.float32),
        in_specs=[
            pl.BlockSpec(memory_space=pltpu.SMEM),
            pl.BlockSpec(memory_space=pltpu.VMEM),
            pl.BlockSpec(memory_space=pl.ANY),
        ],
        out_specs=pl.BlockSpec(memory_space=pltpu.VMEM),
        scratch_shapes=[
            pltpu.VMEM((STEPS, SUBLANES, LANES), jnp.float32),
            pltpu.VMEM((SUBLANES, LANES), jnp.float32),
            pltpu.SMEM((STEPS,), jnp.int32),
            pltpu.SemaphoreType.DMA((STEPS,)),
        ],
        name="table",
    )(pos, psf, residual)


def solve(parts_ref, amps_ref, rows):
    chan_id = lax.axis_index("chan")
    per_chan = DEVICES // NCHAN
    for c in range(NCHAN):
        sums = [parts_ref[c * per_chan + d] for d in range(per_chan)]
        while len(sums) > 1:
            sums = [a + b for a, b in zip(sums[::2], sums[1::2])]
        for g in range(SUBLANES):
            rows[g, c : c + 1, :] = sums[0][g : g + 1, :]
            rows[g, NCHAN + c : NCHAN + c + 1, :] = jnp.zeros((1, LANES), jnp.float32)
    sub = lax.broadcasted_iota(jnp.int32, (SUBLANES, LANES), 0)
    own = sub == chan_id
    amps = []
    for k in range(STEPS):
        line = rows[k // FOLD]
        at = STEPS * (k % FOLD)
        spread = [jnp.broadcast_to(line[:, at + l : at + l + 1], (SUBLANES, LANES)) for l in range(k + 1)]
        value = spread[k]
        for l in range(k):
            value = value - spread[l] * amps[l]
        total = jnp.sum(value, axis=0, keepdims=True)
        amp = 0.25 * (value + total / NCHAN)
        amps.append(jnp.where(sub < NCHAN, amp, 0.0))
        mine = jnp.sum(jnp.where(own, amp, 0.0), axis=0, keepdims=True)
        amps_ref[k] = jnp.broadcast_to(mine, (SUBLANES, LANES))


NEAR = (1, 2, 1, 2)
HALFWAY = (2, 0, 3, 1)


def place(z, y, c):
    return z * 8 + y * 2 + c


def needs(z, y, c, j):
    return 4 * z + y <= 2 * j + c <= 4 * z + y + 16


def near_held(z, y):
    return 4 * NEAR[z] + y


def halfway_held(z, y):
    return 4 * HALFWAY[z] + y if (y < 2) == (z % 2 == 0) else None


def turn(by, held):
    chips = [(z, y) for z in range(4) for y in range(4) if held(z, y) is not None]
    return [
        (place(z, y, c), place(z, (y + by) % 4, c))
        for z, y in chips
        for c in range(2)
        if needs(z, (y + by) % 4, c, held(z, y))
    ]


def climb(moves):
    return [(place(a, y, c), place(b, y, c)) for a, b in moves for y in range(4) for c in range(2)]


OUTER = climb([(1, 0), (2, 3)])
INNER = climb([(2, 1), (1, 2)])
ACROSS = [
    (place(HALFWAY[z], y, c), place(z, y, c))
    for z in range(4)
    for y in range(4)
    for c in range(2)
    if halfway_held(z, y) is not None
]


ACROSS_TWO = [
    (place(HALFWAY[z], (y + 2) % 4, c), place(z, (y + 2) % 4, c))
    for z in range(4)
    for y in range(4)
    for c in range(2)
    if halfway_held(z, y) is not None and needs(z, (y + 2) % 4, c, halfway_held(z, y))
]


def permute(x, pairs):
    return lax.ppermute(x, ROWS, pairs)


def part_kernel(names, halves, late, from_residual, pos_ref, amps_ref, *rest):
    if from_residual:
        parts_ref, (rest, parts, amps_rows, parts_sems) = amps_ref, (rest[:-3], *rest[-3:])
        amps_ref = rest[len(names) + 1]
        rest = (*rest[: len(names) + 1], *rest[len(names) + 2 :])
    count = len(names)
    block_refs, rest = rest[:count], rest[count:]
    base_refs, rest = rest[: 1 if from_residual else len(halves)], rest[1 if from_residual else len(halves) :]
    out_refs, rest = rest[: len(halves)], rest[len(halves) :]
    images, (patch, listed, sems, edge_sems) = rest[: len(halves)], rest[len(halves) :]
    z, y, c = (lax.axis_index(name) for name in ROWS)
    inner = (z == 1) | (z == 2)
    odd = z & 1
    near_slot = jnp.where(z == 0, 4, jnp.where(z == 1, 6, jnp.where(z == 2, 0, 2)))
    far_slot = jnp.where(odd == 0, 8, -2)
    lane = lax.broadcasted_iota(jnp.int32, (SUBLANES, LANES), 1)
    sub = lax.broadcasted_iota(jnp.int32, (SUBLANES, LANES), 0)

    def each_block(act):
        for i, (kind, by) in enumerate(names):
            source = (y - by) & 3
            if kind == "own":
                slot, held = 2 * z + source, None
            elif kind == "far":
                slot, held = far_slot + source, (source >> 1) == odd
            else:
                slot = near_slot + source
                held = None if kind == "near" else inner == (kind == "near_inner")
            slot = jnp.clip(slot, 0, SLOTS - 1)
            rows = pl.ds(pl.multiple_of(EDGE + slot * SHARD, SUBLANES), SHARD)
            copy = pltpu.make_async_copy(block_refs[i], patch.at[rows, :], sems.at[i])
            if held is None:
                act(copy)
            else:
                pl.when(held)(functools.partial(act, copy))

    if from_residual:
        parts_load = pltpu.make_async_copy(parts_ref, parts, parts_sems.at[0])
        parts_load.start()
    each_block(lambda copy: copy.start())
    loads = []
    for n, image in enumerate(images):
        if from_residual and halves[n] == 1:
            image[...] = jnp.zeros(image.shape, jnp.float32)
        else:
            base = base_refs[0 if from_residual else n]
            loads.append(pltpu.make_async_copy(base, image.at[:, pl.ds(0, NCOL)], edge_sems.at[n]))
            loads[-1].start()
    if from_residual:
        parts_load.wait()
        solve(parts, amps_ref, amps_rows)
    each_block(lambda copy: copy.wait())
    for load in loads:
        load.wait()

    def found(first, k):
        start = first - pos_ref[0, k] + HALF
        other = ((start >> 6) ^ c) & 1
        skew = (start & (SHARD - 1)) - other * SHARD
        return skew, (((start >> 6) + other) >> 1) - 2 * z

    def note(first, k, size):
        skew, slot = found(first, k)
        is_late = ((slot >> 1) == jnp.where(odd == 0, 4, 0)) | (slot == near_slot + ((y + 2) & 3))
        listed[size] = k
        return size + ((skew > -SLAB) & (is_late == late)).astype(jnp.int32)

    def peak(image, first, k, counts):
        skew, slot = found(first, k)
        row = EDGE + slot * SHARD + skew
        off = row & (SUBLANES - 1)
        row = row - off
        left = pos_ref[1, k] - HALF
        shift = left & (LANES - 1)
        base = left - shift
        amp = amps_ref[k]
        carried = lane < shift
        upper = sub < SUBLANES - off
        groups = TALL // SUBLANES
        places = [sub + (g * SUBLANES + skew) for g in range(SLAB // SUBLANES)]
        within = [(at >= 0) & (at < SHARD) & counts for at in places]
        back = (SUBLANES - off) & (SUBLANES - 1)
        before = [jnp.zeros((SUBLANES, LANES), jnp.float32)] * (groups - 1)
        for t in range(PATCH // LANES + 1):
            if t < PATCH // LANES:
                raised = []
                for g in range(groups):
                    rows = pl.ds(pl.multiple_of(row + g * SUBLANES, SUBLANES), SUBLANES)
                    raised.append(pltpu.roll(patch[rows, pl.ds(t * LANES, LANES)], back, 0))
                joined = [jnp.where(upper, raised[g], raised[g + 1]) for g in range(groups - 1)]
                turned = [pltpu.roll(x, shift, 1) for x in joined]
            else:
                turned = [jnp.zeros((SUBLANES, LANES), jnp.float32)] * (groups - 1)
            cols = pl.ds(pl.multiple_of(base + t * LANES, LANES), LANES)
            for g in range(groups - 1):
                rows = pl.ds(g * SUBLANES, SUBLANES)
                value = jnp.where(within[g], jnp.where(carried, before[g], turned[g]), 0.0)
                image[rows, cols] = image[rows, cols] - amp * value
            before = turned

    stores = []
    for n, image in enumerate(images):
        half = c if halves[n] == 0 else 1 - c
        first = (4 * z + y) * SHARD + half * SLAB
        size = lax.fori_loop(0, STEPS, functools.partial(note, first), jnp.int32(0))

        def two(i, _, image=image, first=first, size=size):
            second = 2 * i + 1
            peak(image, first, listed[2 * i], True)
            peak(image, first, listed[jnp.minimum(second, size - 1)], second < size)
            return 0

        lax.fori_loop(0, (size + 1) >> 1, two, 0)
        stores.append(pltpu.make_async_copy(image.at[:, pl.ds(0, NCOL)], out_refs[n], edge_sems.at[n]))
        stores[-1].start()
    for store in stores:
        store.wait()


def part(names, halves, late, pos, amps, blocks, bases):
    anywhere = pl.BlockSpec(memory_space=pl.ANY)
    vmem = pl.BlockSpec(memory_space=pltpu.VMEM)
    images = [jax.ShapeDtypeStruct((SLAB, NCOL), jnp.float32)] * len(halves)
    solved = [] if late else [jax.ShapeDtypeStruct((STEPS, SUBLANES, LANES), jnp.float32)]
    solving = [
        pltpu.VMEM((DEVICES, SUBLANES, LANES), jnp.float32),
        pltpu.VMEM((SUBLANES, SUBLANES, LANES), jnp.float32),
        pltpu.SemaphoreType.DMA((1,)),
    ]
    return pl.pallas_call(
        functools.partial(part_kernel, names, halves, late, not late),
        out_shape=solved + images,
        in_specs=[pl.BlockSpec(memory_space=pltpu.SMEM), vmem if late else anywhere]
        + [anywhere] * (len(blocks) + len(bases)),
        out_specs=[vmem] * len(solved) + [anywhere] * len(halves),
        scratch_shapes=[pltpu.VMEM((SLAB, NCOL + LANES), jnp.float32)] * len(halves)
        + [
            pltpu.VMEM((2 * EDGE + SLOTS * SHARD, PATCH), jnp.float32),
            pltpu.SMEM((STEPS + SUBLANES,), jnp.int32),
            pltpu.SemaphoreType.DMA((len(names),)),
            pltpu.SemaphoreType.DMA((len(halves),)),
        ]
        + ([] if late else solving),
        compiler_params=pltpu.CompilerParams(vmem_limit_bytes=PART_VMEM),
    )(pos, amps, *blocks, *bases)


def join_kernel(mine_ref, other_ref, out_ref, *rest):
    piece_refs, (mine, other, sems, piece_sems) = rest[: len(PIECES)], rest[len(PIECES) :]
    chan_id = lax.axis_index("chan")

    def cols(ahead):
        return pl.ds(pl.multiple_of(((chan_id + ahead) & (NCHAN - 1)) * QUARTER, QUARTER), QUARTER)

    def load(ahead, n):
        src, dst = ((mine_ref, mine), (other_ref, other))[n]
        return pltpu.make_async_copy(src.at[:, cols(ahead)], dst.at[ahead], sems.at[n, ahead])

    order = (2, 1, 3, 0)
    for ahead in order:
        load(ahead, 0).start()
        load(ahead, 1).start()
    stores = []
    for ahead in order:
        load(ahead, 0).wait()
        load(ahead, 1).wait()
        mine[ahead] = mine[ahead] + other[ahead]
        stores.append(pltpu.make_async_copy(mine.at[ahead], out_ref.at[:, cols(ahead)], sems.at[2, ahead]))
        stores[-1].start()
        for i, (where, top, tall) in enumerate(PIECES):
            if where == ahead:
                src = mine.at[ahead, pl.ds(top, tall), :]
                stores.append(pltpu.make_async_copy(src, piece_refs[i], piece_sems.at[i]))
                stores[-1].start()
    for store in stores:
        store.wait()


def join(mine, other):
    anywhere = pl.BlockSpec(memory_space=pl.ANY)
    return pl.pallas_call(
        join_kernel,
        out_shape=[
            jax.ShapeDtypeStruct((SLAB, NCOL), jnp.float32),
            *(jax.ShapeDtypeStruct((tall, QUARTER), jnp.float32) for _, _, tall in PIECES),
        ],
        in_specs=[anywhere] * 2,
        out_specs=[anywhere] * (len(PIECES) + 1),
        scratch_shapes=[
            pltpu.VMEM((NCHAN, SLAB, QUARTER), jnp.float32),
            pltpu.VMEM((NCHAN, SLAB, QUARTER), jnp.float32),
            pltpu.SemaphoreType.DMA((3, NCHAN)),
            pltpu.SemaphoreType.DMA((len(PIECES),)),
        ],
        compiler_params=pltpu.CompilerParams(vmem_limit_bytes=JOIN_VMEM),
        name="join",
    )(mine, other)


def channel_sum(pieces):
    mine, right_top, right_low, far_top, far_low, left_top, left_low = pieces

    def shift(x, by):
        return lax.ppermute(x, "chan", [(i, (i + by) % NCHAN) for i in range(NCHAN)])

    far_top, far_low = shift(far_top, 1), shift(far_low, 3)
    from_left_low, from_right_top = shift(right_low, 1), shift(left_top, 3)
    from_left_top, from_right_low = shift(right_top + far_top, 1), shift(left_low + far_low, 3)
    return mine + jnp.concatenate([from_left_top + from_right_top, from_left_low + from_right_low], 0)


def cycle(residual, psf, positions):
    nrows = lax.axis_size(ROWS)
    slab, ncols = residual.shape[1:]
    z = lax.axis_index("rows_0")
    outer = (z == 0) | (z == 3)
    pos = positions.T
    own = psf[0]
    to_outer, to_inner = permute(own, OUTER), permute(own, INNER)
    own1, own3, own2 = (permute(own, turn(by, lambda z, y: 4 * z + y)) for by in (1, 3, 2))
    far = permute(own, ACROSS)
    parts = table(pos, own, residual[0])
    near = jnp.where(outer, to_outer, to_inner)
    near1, near3 = (permute(near, turn(by, near_held)) for by in (1, 3))
    parts = lax.all_to_all(parts, CHAN_ROWS, 0, 0, tiled=True)
    far1, far3 = (permute(far, turn(by, halfway_held)) for by in (1, 3))
    far2 = permute(own2, ACROSS_TWO)
    near2_outer, near2_inner = permute(own2, OUTER), permute(own2, INNER)
    early = (own, own1, own2, own3, near, near1, near3)
    amps, mine, yours = part(EARLY, (0, 1), False, pos, parts, early, (residual[0],))
    rest = (near2_outer, near2_inner, far, far1, far2, far3)
    (yours,) = part(LATE, (1,), True, pos, amps, rest, (yours,))
    other = lax.ppermute(yours, "rows_2", [(0, 1), (1, 0)])
    (mine,) = part(LATE, (0,), True, pos, amps, rest, (mine,))
    image, *pieces = join(mine, other)
    summed = channel_sum(pieces)
    square = jnp.broadcast_to(jnp.sum(summed * summed), (DEVICES, 1, LANES))
    total = jnp.sum(lax.all_to_all(square, CHAN_ROWS, 0, 0, tiled=True)[:, 0, 0])
    count = slab * nrows * ncols
    normalized = summed * lax.rsqrt(total / count + 1e-06)
    return (image[None], normalized)


def solution(mesh):
    finer = Mesh(
        mesh.devices.reshape(mesh.shape["chan"], 4, 4, 2), ("chan", "rows_0", "rows_1", "rows_2")
    )
    return jax.shard_map(
        cycle,
        mesh=finer,
        in_specs=(P("chan", ROWS, None), P("chan", ROWS, None), P()),
        out_specs=(P("chan", ROWS, None), P(ROWS, "chan")),
        check_vma=False,
    )
```
